512 devices in a mesh: dp: 32 (over z, x_lo, core), mp: 2 (over x_hi), pre: 8 (over y).
Axes of the slice: x: 4 (x_hi: 2, x_lo: 2; x = x_hi * 2 + x_lo), y: 8, z: 8, core: 2. Of those that a mesh axis runs over, the one named last changes fastest.
Arguments:
- activations: bfloat16 [49152, 1024], P('dp'), may hold values from -6 to 6
- grad_output: bfloat16 [49152, 4096], P('dp', ('mp', 'pre')), may hold values from -0.02734375 to 0.02734375
- left_old: float32 [1024, 1024], P(('mp', 'pre'), 'dp'), may hold values from -1 to 9, as said below
- right_old: float32 [4096, 4096], P(('mp', 'pre'), 'dp'), may hold values from -1 to 9, as said below
- probe_left: float32 [1024], replicated, may hold values from -6 to 6
- probe_right: float32 [4096], replicated, may hold values from -6 to 6
Outputs:
- left_new: float32 [1024, 1024], P(('mp', 'pre'), 'dp')
- right_new: float32 [4096, 4096], P(('mp', 'pre'), 'dp')
- update: float32 [1024, 4096], P('dp', ('mp', 'pre'))
The draws below stay inside these ranges and needn't reach their ends.
Inputs may be any that keep to these rules, and one draw needn't show every extreme that they name: `left_old`: symmetric and positive definite. `right_old`: symmetric and positive definite.
All inputs are finite; a program needn't handle non-finite values.
Results may differ from the reference program's by a relative error of at most 0.0003.
Values sent between devices are 32-bit elements; how exact they have to be, the bound alone decides.
A program may use at most 64 MiB of HBM per device.

```python
import math
import jax
import jax.numpy as jnp
from jax import lax

D = 1024
FF = 4096
TOKENS = 49152


def symmetric_draw(key, order):
    first_key, second_key = jax.random.split(jax.random.fold_in(key, 7))
    random_part = jax.random.normal(first_key, (order, order), jnp.float32) * (0.5 / math.sqrt(order))
    off_part = (random_part + random_part.T) * 0.5
    diagonal = jax.random.uniform(second_key, (order,), jnp.float32, 1.0, 2.0)
    return off_part + jnp.diag(diagonal)


def draw_left_old(key, part):
    return symmetric_draw(key, D)


def draw_right_old(key, part):
    return symmetric_draw(key, FF)


def level_of(own_key, shape, pieces, low, top_value):
    def one(dim, parts):
        heights = jax.random.uniform(jax.random.fold_in(jax.random.fold_in(own_key, 6), dim), (parts,), jnp.float32, low / len(pieces), top_value / len(pieces))
        return jnp.repeat(jnp.exp(heights), shape[dim] // parts).reshape((-1,) + (1,) * (len(shape) - dim - 1))

    level = one(*pieces[0])
    for cut in pieces[1:]:
        level = level * one(*cut)
    return level


def normal_values(key, extent, spread, reach, cuts=(), held_as=jnp.bfloat16):
    drawn = spread * jax.random.normal(key, extent, jnp.float32)
    if cuts:
        drawn = drawn * level_of(key, extent, cuts, -0.22, 0.18)
    return jnp.clip(drawn, -reach, reach).astype(held_as)


def setup_inputs(seed: int = 0) -> dict:
    splits = jax.random.split(jax.random.key(seed), 7)
    return {
        "activations": normal_values(splits[0], (TOKENS, D), 1.0, 6.0, ((0, 32),)),
        "grad_output": normal_values(splits[1], (TOKENS, FF), TOKENS ** -0.5, 0.02734375, ((0, 32), (1, 16))),
        "left_old": draw_left_old(jax.random.fold_in(splits[6], 71), 0),
        "right_old": draw_right_old(jax.random.fold_in(splits[6], 71), 0),
        "probe_left": normal_values(splits[4], (D,), 1.0, 6.0, (), jnp.float32),
        "probe_right": normal_values(splits[5], (FF,), 1.0, 6.0, (), jnp.float32),
    }


beta_decay = 0.9
norm_floor = 1e-06

def length_of(vector):
    return jnp.sqrt(jnp.sum(vector * vector) + norm_floor)

def largest(matrix, probe):
    highest = lax.Precision.HIGHEST
    first_image = jnp.dot(matrix, probe, precision=highest, preferred_element_type=jnp.float32)
    unit_vector = first_image / length_of(first_image)
    second_image = jnp.dot(matrix, unit_vector, precision=highest, preferred_element_type=jnp.float32)
    return length_of(second_image)

def reference(activations, grad_output, left_old, right_old, probe_left, probe_right):
    highest = lax.Precision.HIGHEST
    gradient = jnp.dot(activations.T, grad_output, preferred_element_type=jnp.float32)
    left_new = beta_decay * left_old + jnp.dot(gradient, gradient.T, precision=highest, preferred_element_type=jnp.float32) / FF
    right_new = beta_decay * right_old + jnp.dot(gradient.T, gradient, precision=highest, preferred_element_type=jnp.float32) / D
    top_left = largest(left_new, probe_left)
    top_right = largest(right_new, probe_right)
    half_step = (5.0 * gradient - jnp.dot(left_new, gradient, precision=highest, preferred_element_type=jnp.float32) / top_left) * 0.25
    update = (5.0 * half_step - jnp.dot(half_step, right_new, precision=highest, preferred_element_type=jnp.float32) / top_right) * 0.25
    update = update * (top_left * top_right) ** (-0.25)
    return (left_new, right_new, update)
```

```python
import functools

import jax
import jax.numpy as jnp
from jax import lax
from jax.experimental import pallas as pl
from jax.experimental.pallas import tpu as pltpu
from jax.sharding import PartitionSpec as P

MESH = pl.DeviceIdType.MESH
F32 = jnp.float32
BF16 = jnp.bfloat16

DECAY = 0.9
FLOOR = 1e-06
SLAB = 64
HALF = 128
COPIES = 176

NN = (((1,), (0,)), ((), ()))
NT = (((1,), (1,)), ((), ()))
TN = (((0,), (0,)), ((), ()))


def far_first(n):
    return sorted(range(1, n), key=lambda o: -min(o, n - o))


def near_first(n):
    return sorted(range(1, n), key=lambda o: min(o, n - o))


def halves(v):
    high = v.astype(BF16)
    return high, (v - high.astype(F32)).astype(BF16)


def dot3(a, b, dims):
    (ah, al), (bh, bl) = a, b
    dot = functools.partial(lax.dot_general, dimension_numbers=dims, preferred_element_type=F32)
    return dot(ah, bh) + (dot(ah, bl) + dot(al, bh))


class Net:
    def __init__(self, send_sem, recv_sem):
        self.send_sem, self.recv_sem, self.used, self.sent = send_sem, recv_sem, 0, []

    def slot(self):
        self.used += 1
        assert self.used <= COPIES
        return self.used - 1

    def copy(self, i, src, dst, device):
        return pltpu.make_async_remote_copy(
            src_ref=src,
            dst_ref=dst,
            send_sem=self.send_sem.at[i],
            recv_sem=self.recv_sem.at[i],
            device_id=device,
            device_id_type=MESH,
        )

    def send(self, i, src, dst, device):
        copy = self.copy(i, src, dst, device)
        copy.start()
        self.sent.append(copy)

    def arrive(self, i, dst, device):
        self.copy(i, dst, dst, device).wait_recv()

    def finish(self):
        for copy in self.sent:
            copy.wait_send()


def kernel(
    nz,
    ny,
    ff,
    act,
    dy,
    left_old,
    right_old,
    p_left,
    p_right,
    left_out,
    right_out,
    update_out,
    part,
    rc,
    xs,
    rx,
    zs,
    rz,
    grad,
    part2,
    rc2,
    xs2,
    rx2,
    zs2,
    rz2,
    prod,
    gown,
    panel,
    rtile,
    lpart,
    lr,
    lsum,
    lx,
    lrow,
    square,
    square2,
    abuf,
    arecv,
    azrecv,
    bbuf,
    brecv,
    byrecv,
    cbuf,
    crecv,
    czrecv,
    send_sem,
    recv_sem,
):
    d_model = nz * 2 * SLAB
    rows_l = d_model // 128
    dp, mp, pre = lax.axis_index("dp"), lax.axis_index("mp"), lax.axis_index("pre")
    z, xl, c = dp // 4, (dp // 2) % 2, dp % 2
    a = mp * ny + pre
    b = z * 2 + xl
    on_diagonal = a == b

    core_peer = (dp + 1 - 2 * c, mp, pre)
    x_peer = (dp + 2 - 4 * xl, mp, pre)
    hi_peer = (dp, 1 - mp, pre)
    flip_peer = (a * 2 + c, b // ny, b % ny)

    def z_at(o):
        return (z + o) % nz

    def z_peer(o):
        return (z_at(o) * 4 + xl * 2 + c, mp, pre)

    def y_at(o):
        return (pre + o) % ny

    def y_peer(o):
        return (dp, mp, y_at(o))

    net = Net(send_sem, recv_sem)

    barrier = pltpu.get_barrier_semaphore()

    def greet(device):
        pl.semaphore_signal(barrier, inc=1, device_id=device, device_id_type=MESH)

    greet(core_peer)
    greet(x_peer)
    greet(hi_peer)
    for o in range(1, nz):
        greet(z_peer(o))
    for o in range(1, ny):
        greet(y_peer(o))

    @pl.when(jnp.logical_not(on_diagonal))
    def _():
        greet(flip_peer)

    def slab_rows(z_, xl_):
        return pl.ds(pl.multiple_of((z_ * 2 + xl_) * SLAB, SLAB), SLAB)

    def pair_rows(z_):
        return pl.ds(pl.multiple_of(z_ * 2 * SLAB, 2 * SLAB), 2 * SLAB)

    def half_cols(c_):
        return pl.ds(pl.multiple_of(c_ * HALF, HALF), HALF)

    mine, other = half_cols(c), half_cols(1 - c)
    z_order = far_first(nz) + [0]

    class Scatter:
        def __init__(self, part, rc, xs, rx, zs, rz):
            self.part, self.rc, self.xs, self.rx, self.zs, self.rz = part, rc, xs, rx, zs, rz
            self.ic = [net.slot() for _ in range(nz)]
            self.ix = [net.slot() for _ in range(nz)]
            self.iz = [net.slot() for _ in range(nz)]

        def block(self, o, value):
            rows = pair_rows(z_at(o))
            self.part[rows, :] = value
            net.send(self.ic[o], self.part.at[rows, other], self.rc.at[rows, :], core_peer)

        def over_x(self, o):
            rows = pair_rows(z_at(o))
            net.arrive(self.ic[o], self.rc.at[rows, :], core_peer)
            theirs = slab_rows(z_at(o), 1 - xl)
            self.xs[o] = self.part[theirs, mine] + self.rc[theirs, :]
            net.send(self.ix[o], self.xs.at[o], self.rx.at[o], x_peer)

        def over_z(self, o):
            net.arrive(self.ix[o], self.rx.at[o], x_peer)
            ours = slab_rows(z_at(o), xl)
            self.zs[o] = self.part[ours, mine] + self.rc[ours, :] + self.rx[o]
            if o:
                net.send(self.iz[o], self.zs.at[o], self.rz.at[o], z_peer(o))

        def total(self):
            value = self.zs[0]
            for o in near_first(nz):
                net.arrive(self.iz[o], self.rz.at[o], z_peer(o))
                value = value + self.rz[o]
            return value

    class Gather:
        def __init__(self, full):
            self.full = full
            self.ic = [net.slot() for _ in range(nz)]
            self.ix = [net.slot() for _ in range(nz)]
            self.iz = [net.slot() for _ in range(nz)]

        def over_z(self, value):
            rows = slab_rows(z, xl)
            self.full[rows, mine] = value
            chunk = self.full.at[rows, mine]
            for o in far_first(nz):
                net.send(self.iz[o], chunk, chunk, z_peer(o))
            net.send(self.ix[0], chunk, chunk, x_peer)

        def over_x(self, o):
            chunk = self.full.at[slab_rows(z_at(nz - o), xl), mine]
            net.arrive(self.iz[o], chunk, z_peer(nz - o))
            net.send(self.ix[o], chunk, chunk, x_peer)

        def over_core(self, o):
            z_ = z_at(nz - o)
            net.arrive(self.ix[o], self.full.at[slab_rows(z_, 1 - xl), mine], x_peer)
            pair = self.full.at[pair_rows(z_), mine]
            net.send(self.ic[o], pair, pair, core_peer)

        def landed(self, o):
            net.arrive(self.ic[o], self.full.at[pair_rows(z_at(nz - o)), other], core_peer)

    first = Scatter(part, rc, xs, rx, zs, rz)
    gather = Gather(grad)

    def grad_block(o):
        cols = pl.ds(pl.multiple_of(z_at(o) * 128, 128), 128)
        return lax.dot_general(act[:, cols], dy[...], TN, preferred_element_type=F32)

    first_value = grad_block(z_order[0])
    count = 3 + (nz - 1) + (ny - 1)
    pl.semaphore_wait(barrier, count + jnp.where(on_diagonal, 0, 1))
    first.block(z_order[0], first_value)
    for o in z_order[1:]:
        first.block(o, grad_block(o))
    for o in z_order:
        first.over_x(o)
    for o in z_order:
        first.over_z(o)
    gown[...] = first.total()

    i_flip = net.slot()
    iy = [net.slot() for _ in range(ny)]
    ih = [net.slot() for _ in range(ny)]

    def a_rows(mp_, y_):
        return pl.ds(pl.multiple_of((mp_ * ny + y_) * SLAB, SLAB), SLAB)

    own_rows = a_rows(mp, pre)
    flip_rows = pl.ds(pl.multiple_of(b * SLAB, SLAB), SLAB)

    @pl.when(jnp.logical_not(on_diagonal))
    def _():
        net.copy(i_flip, gown, panel.at[flip_rows, :], flip_peer).start()

    @pl.when(on_diagonal)
    def _():
        panel[own_rows, :] = gown[...]

    gather.over_z(gown[...])
    for o in near_first(nz)[: nz // 2]:
        gather.over_x(o)

    @pl.when(jnp.logical_not(on_diagonal))
    def _():
        net.copy(i_flip, gown, panel.at[own_rows, :], flip_peer).wait_recv()

    own_panel = panel.at[own_rows, :]
    for o in far_first(ny):
        net.send(iy[o], own_panel, own_panel, y_peer(o))
    net.send(ih[0], own_panel, own_panel, hi_peer)
    for o in near_first(nz)[nz // 2 :]:
        gather.over_x(o)
    for o in [0] + near_first(nz):
        gather.over_core(o)

    def panel_over_hi(o):
        chunk = panel.at[a_rows(mp, y_at(ny - o)), :]
        net.arrive(iy[o], chunk, y_peer(ny - o))
        net.send(ih[o], chunk, chunk, hi_peer)

    for o in near_first(ny)[: ny // 2]:
        panel_over_hi(o)
    for o in [0] + near_first(nz):
        gather.landed(o)

    il = [net.slot() for _ in range(ny)]
    ilx = net.slot()
    ilg = [net.slot() for _ in range(ny)]
    grad_high, grad_low = halves(grad[...])
    own_grad = grad[pl.ds(pl.multiple_of(dp * 32, 32), 32), :]
    lpart[...] = dot3(halves(own_grad), (grad_high, grad_low), NT) * (1.0 / ff)
    square[...] = jnp.zeros_like(square)
    square[pl.ds(pl.multiple_of((a % 2) * SLAB, SLAB), SLAB), pl.ds(0, 32)] = (
        left_old[...] * DECAY
    )
    old_lanes = pl.ds(pl.multiple_of((a // 2) * 128, 128), 128)
    square2[...] = square[...].T
    lpart[:, old_lanes] += square2[pl.ds(0, 32), :]

    def l_lanes(y_):
        return pl.ds(pl.multiple_of(y_ * 128, 128), 128)

    for o in far_first(ny):
        net.send(il[o], lpart.at[:, l_lanes(y_at(o))], lr.at[o], y_peer(o))
    for o in near_first(ny)[ny // 2 :]:
        panel_over_hi(o)
    total = lpart[:, l_lanes(pre)]
    for o in near_first(ny):
        net.arrive(il[o], lr.at[o], y_peer(o))
        total = total + lr[o]
    lsum[...] = total
    net.send(ilx, lsum, lx, hi_peer)
    for o in [0] + near_first(ny):
        net.arrive(ih[o], panel.at[a_rows(1 - mp, y_at(ny - o)), :], hi_peer)

    panel_high, panel_low = halves(panel[...])
    panel_t = halves(panel[...].T)
    gram = dot3(panel_t, (grad_high, grad_low), NN)
    rtile[...] = right_old[...].T * DECAY + gram * (1.0 / d_model)

    net.arrive(ilx, lx, hi_peer)
    lrow[:, l_lanes(pre)] = lsum[...] + lx[...]
    own_lanes = lrow.at[:, l_lanes(pre)]
    for o in far_first(ny):
        net.send(ilg[o], own_lanes, own_lanes, y_peer(o))

    second = Scatter(part2, rc2, xs2, rx2, zs2, rz2)
    gather2 = Gather(prod)
    rt_split = halves(rtile[...])
    part_panel = (panel_high, panel_low)

    def prod_block(o):
        rows = pair_rows(z_at(o))
        return dot3(halves(panel[rows, :]), rt_split, NN)

    for o in z_order:
        second.block(o, prod_block(o))
    for o in z_order:
        second.over_x(o)

    for o in near_first(ny):
        net.arrive(ilg[o], lrow.at[:, l_lanes(y_at(ny - o))], y_peer(ny - o))
    square[...] = jnp.zeros_like(square)
    square[pl.ds(0, rows_l), :] = p_left[...]
    lane = lax.broadcasted_iota(jnp.int32, (128, 128), 1)
    column = jnp.sum(jnp.where(lane == dp // 4, square[...].T, 0.0), axis=1, keepdims=True)
    square2[...] = jnp.broadcast_to(column, (128, 128))
    p_col = square2[pl.ds(pl.multiple_of((dp % 4) * 32, 32), 32), pl.ds(0, 1)]
    first_left = jnp.sum(lrow[...] * p_col, axis=0, keepdims=True)
    p_row = jnp.broadcast_to(p_right[pl.ds(dp, 1), :], (8, 128))
    first_right = dot3(halves(p_row), rt_split, NN)
    abuf[0] = jnp.zeros_like(abuf[0])
    for j in range(rows_l):
        abuf[0, pl.ds(j, 1), :] = first_left[:, j * 128 : (j + 1) * 128]
    abuf[0, pl.ds(8, 1), :] = first_right[0:1, :128]
    abuf[0, pl.ds(9, 1), :] = first_right[0:1, 128:]

    class Sum:
        def __init__(self, buf, recv, zrecv):
            self.buf, self.recv, self.zrecv = buf, recv, zrecv
            self.ic, self.ix = net.slot(), net.slot()
            self.iz = [net.slot() for _ in range(nz)]

        def over_core(self):
            net.send(self.ic, self.buf.at[0], self.recv.at[0], core_peer)

        def over_x(self):
            net.arrive(self.ic, self.recv.at[0], core_peer)
            self.buf[1] = self.buf[0] + self.recv[0]
            net.send(self.ix, self.buf.at[1], self.recv.at[1], x_peer)

        def over_z(self):
            net.arrive(self.ix, self.recv.at[1], x_peer)
            self.buf[2] = self.buf[1] + self.recv[1]
            for o in far_first(nz):
                net.send(self.iz[o], self.buf.at[2], self.zrecv.at[o], z_peer(o))

        def total(self):
            value = self.buf[2]
            for o in near_first(nz):
                net.arrive(self.iz[o], self.zrecv.at[o], z_peer(o))
                value = value + self.zrecv[o]
            return value

    asum = Sum(abuf, arecv, azrecv)
    csum = Sum(cbuf, crecv, czrecv)
    asum.over_core()
    for o in z_order[: nz // 2]:
        second.over_z(o)
    asum.over_x()
    for o in z_order[nz // 2 :]:
        second.over_z(o)
    asum.over_z()
    gather2.over_z(second.total())

    images = asum.total()
    f_left = images[0:rows_l, :]
    norm_left = jnp.sqrt(
        jnp.sum(jnp.sum(f_left * f_left, axis=1, keepdims=True), axis=0, keepdims=True) + FLOOR
    )
    unit_left = f_left / norm_left
    second_left = jnp.zeros((32, 1), F32)
    for j in range(rows_l):
        second_left = second_left + jnp.sum(
            lrow[:, j * 128 : (j + 1) * 128] * unit_left[j : j + 1, :], axis=1, keepdims=True
        )
    left_square = jnp.sum(second_left * second_left, axis=0, keepdims=True)
    f_low, f_high = images[8:9, :], images[9:10, :]
    right_square = jnp.sum(f_low * f_low + f_high * f_high, axis=1, keepdims=True)
    f_row = jnp.concatenate([f_low, f_high], axis=1)
    second_right = dot3(halves(jnp.broadcast_to(f_row, (8, 2 * HALF))), rt_split, NT)
    row = lax.broadcasted_iota(jnp.int32, (8, 128), 0)
    bbuf[0] = jnp.where(row == 0, second_right, right_square)
    ibx = net.slot()
    iby = [net.slot() for _ in range(ny)]
    net.send(ibx, bbuf.at[0], brecv, hi_peer)
    for o in near_first(nz)[: nz // 2]:
        gather2.over_x(o)
    net.arrive(ibx, brecv, hi_peer)
    bbuf[1] = bbuf[0] + brecv[...]
    for o in far_first(ny):
        net.send(iby[o], bbuf.at[1], byrecv.at[o], y_peer(o))
    for o in near_first(nz)[nz // 2 :]:
        gather2.over_x(o)
    whole = bbuf[1]
    for o in near_first(ny):
        net.arrive(iby[o], byrecv.at[o], y_peer(o))
        whole = whole + byrecv[o]
    norm_right = jnp.sqrt(whole[1:2, 0:1] + FLOOR)
    scaled = whole[0:1, :] / norm_right
    tops = jnp.sum(scaled * scaled, axis=1, keepdims=True)
    cbuf[0] = jnp.where(row == 0, tops, left_square)
    csum.over_core()
    for o in ([0] + near_first(nz))[: nz // 2]:
        gather2.over_core(o)
    csum.over_x()
    for o in ([0] + near_first(nz))[nz // 2 :]:
        gather2.over_core(o)
    csum.over_z()

    right_out[...] = rtile[...].T
    square[...] = jnp.zeros_like(square)
    square[pl.ds(0, 32), :] = lrow[:, old_lanes]
    square2[...] = square[...].T
    left_out[...] = square2[pl.ds(pl.multiple_of((a % 2) * SLAB, SLAB), SLAB), pl.ds(0, 32)]

    tops = csum.total()
    top_right = jnp.sqrt(tops[0:1, 0:1] + FLOOR)
    top_left = jnp.sqrt(tops[1:2, 0:1] + FLOOR)
    for o in [0] + near_first(nz):
        gather2.landed(o)
    mixed = 5.0 * grad[...] - prod[...] / top_right
    left_term = dot3(halves(lrow[...]), halves(mixed), NN)
    own32 = pl.ds(pl.multiple_of(dp * 32, 32), 32)
    own = 5.0 * grad[own32, :] - prod[own32, :] / top_right
    scale = lax.rsqrt(jnp.sqrt(top_left * top_right)) * 0.0625
    update_out[...] = (5.0 * own - left_term / top_left) * scale

    @pl.when(jnp.logical_not(on_diagonal))
    def _():
        net.copy(i_flip, gown, panel.at[flip_rows, :], flip_peer).wait_send()

    net.finish()


def step(nz, ny, ff, activations, grad_output, left_old, right_old, probe_left, probe_right):
    d_model = activations.shape[1]
    block = grad_output.shape[1]
    vmem = pltpu.VMEM

    def scatter_bufs():
        return [
            vmem((d_model, block), F32),
            vmem((d_model, HALF), F32),
            vmem((nz, SLAB, HALF), F32),
            vmem((nz, SLAB, HALF), F32),
            vmem((nz, SLAB, HALF), F32),
            vmem((nz, SLAB, HALF), F32),
            vmem((d_model, block), F32),
        ]

    scratch = [
        *scatter_bufs(),
        *scatter_bufs(),
        vmem((SLAB, HALF), F32),
        vmem((d_model, HALF), F32),
        vmem((HALF, block), F32),
        vmem((32, d_model), F32),
        vmem((ny, 32, 128), F32),
        vmem((32, 128), F32),
        vmem((32, 128), F32),
        vmem((32, d_model), F32),
        vmem((128, 128), F32),
        vmem((128, 128), F32),
        vmem((3, 16, 128), F32),
        vmem((2, 16, 128), F32),
        vmem((nz, 16, 128), F32),
        vmem((2, 8, 128), F32),
        vmem((8, 128), F32),
        vmem((ny, 8, 128), F32),
        vmem((3, 8, 128), F32),
        vmem((2, 8, 128), F32),
        vmem((nz, 8, 128), F32),
        pltpu.SemaphoreType.DMA((COPIES,)),
        pltpu.SemaphoreType.DMA((COPIES,)),
    ]
    spec = pl.BlockSpec(memory_space=pltpu.VMEM)
    return pl.pallas_call(
        functools.partial(kernel, nz, ny, ff),
        out_shape=(
            jax.ShapeDtypeStruct(left_old.shape, F32),
            jax.ShapeDtypeStruct(right_old.shape, F32),
            jax.ShapeDtypeStruct((d_model // (4 * nz), block), F32),
        ),
        in_specs=[spec] * 6,
        out_specs=(spec,) * 3,
        scratch_shapes=scratch,
        compiler_params=pltpu.CompilerParams(
            collective_id=0, has_side_effects=True, vmem_limit_bytes=48 * 1024 * 1024
        ),
        name="shampoo",
    )(
        activations,
        grad_output,
        left_old,
        right_old,
        probe_left.reshape(-1, 128),
        probe_right.reshape(-1, 128),
    )


def solution(mesh):
    nz = mesh.shape["dp"] // 4
    ny = mesh.shape["pre"]
    in_specs = (
        P("dp", None),
        P("dp", ("mp", "pre")),
        P(("mp", "pre"), "dp"),
        P(("mp", "pre"), "dp"),
        P(),
        P(),
    )
    out_specs = (P(("mp", "pre"), "dp"), P(("mp", "pre"), "dp"), P("dp", ("mp", "pre")))
    ff = 2 * ny * 2 * HALF
    return jax.shard_map(
        functools.partial(step, nz, ny, ff),
        mesh=mesh,
        in_specs=in_specs,
        out_specs=out_specs,
        check_vma=False,
    )
```

```python
import functools

import jax
import jax.numpy as jnp
from jax import lax
from jax.experimental import pallas as pl
from jax.experimental.pallas import tpu as pltpu
from jax.sharding import PartitionSpec as P

MESH = pl.DeviceIdType.MESH
F32 = jnp.float32
BF16 = jnp.bfloat16

DECAY = 0.9
FLOOR = 1e-06
SLAB = 64
HALF = 128
COPIES = 216

NN = (((1,), (0,)), ((), ()))
NT = (((1,), (1,)), ((), ()))
TN = (((0,), (0,)), ((), ()))


def far_first(n):
    return sorted(range(1, n), key=lambda o: -min(o, n - o))


def near_first(n):
    return sorted(range(1, n), key=lambda o: min(o, n - o))


def halves(v):
    high = v.astype(BF16)
    return high, (v - high.astype(F32)).astype(BF16)


def dot3(a, b, dims):
    (ah, al), (bh, bl) = a, b
    dot = functools.partial(lax.dot_general, dimension_numbers=dims, preferred_element_type=F32)
    return dot(ah, bh) + (dot(ah, bl) + dot(al, bh))


class Net:
    def __init__(self, send_sem, recv_sem):
        self.send_sem, self.recv_sem, self.used, self.sent = send_sem, recv_sem, 0, []

    def slot(self):
        self.used += 1
        assert self.used <= COPIES
        return self.used - 1

    def copy(self, i, src, dst, device):
        return pltpu.make_async_remote_copy(
            src_ref=src,
            dst_ref=dst,
            send_sem=self.send_sem.at[i],
            recv_sem=self.recv_sem.at[i],
            device_id=device,
            device_id_type=MESH,
        )

    def send(self, i, src, dst, device):
        copy = self.copy(i, src, dst, device)
        copy.start()
        self.sent.append(copy)

    def arrive(self, i, dst, device):
        self.copy(i, dst, dst, device).wait_recv()

    def finish(self):
        for copy in self.sent:
            copy.wait_send()


def kernel(
    nz,
    ny,
    ff,
    act_hbm,
    dy_hbm,
    left_hbm,
    right_hbm,
    p_left_hbm,
    p_right_hbm,
    left_out,
    right_out,
    update_out,
    act,
    dy,
    left_old,
    right_old,
    p_left,
    p_right,
    part,
    rc,
    xs,
    rx,
    zs,
    rz,
    grad,
    part2,
    rc2,
    xs2,
    rx2,
    zs2,
    rz2,
    prod,
    gown,
    panel,
    rtile,
    lpart,
    lr,
    lsum,
    lx,
    lrow,
    abuf,
    arecv,
    azrecv,
    hbuf,
    hrecv,
    hyrecv,
    fbuf,
    frecv,
    fzrecv,
    bbuf,
    brecv,
    byrecv,
    cbuf,
    crecv,
    czrecv,
    send_sem,
    recv_sem,
    load_sem,
):
    d_model = nz * 2 * SLAB
    rows_l = d_model // 128
    dp, mp, pre = lax.axis_index("dp"), lax.axis_index("mp"), lax.axis_index("pre")
    z, xl, c = dp // 4, (dp // 2) % 2, dp % 2
    a = mp * ny + pre
    b = z * 2 + xl
    core_peer = (dp + 1 - 2 * c, mp, pre)
    x_peer = (dp + 2 - 4 * xl, mp, pre)
    hi_peer = (dp, 1 - mp, pre)

    turn = (z - a // 2 + ny // 2 + nz) % nz
    goal_hi = jnp.where(xl == a % 2, mp, 1 - mp)
    flip_to = (a * 2 + c, goal_hi, (pre + turn) % ny)
    came = (z + pre - b % ny + ny // 2 + nz) % nz
    came_lo = jnp.where(mp == b // ny, xl, 1 - xl)
    flip_from = (came * 4 + came_lo * 2 + c, b // ny, b % ny)
    flip_to_2 = (a * 2 + c, 1 - goal_hi, (pre + turn) % ny)
    flip_from_2 = (came * 4 + (1 - came_lo) * 2 + c, b // ny, b % ny)

    def z_at(o):
        return (z + o) % nz

    def z_peer(o):
        return (z_at(o) * 4 + xl * 2 + c, mp, pre)

    def y_at(o):
        return (pre + o) % ny

    def y_peer(o):
        return (dp, mp, y_at(o))

    net = Net(send_sem, recv_sem)

    barrier = pltpu.get_barrier_semaphore()

    def greet(device):
        pl.semaphore_signal(barrier, inc=1, device_id=device, device_id_type=MESH)

    greet(core_peer)
    greet(x_peer)
    greet(hi_peer)
    for o in range(1, nz):
        greet(z_peer(o))
    for o in range(1, ny):
        greet(y_peer(o))

    greet(flip_from)
    greet(flip_from_2)

    loads = []

    def load(src, dst):
        copy = pltpu.make_async_copy(src, dst, load_sem.at[len(loads)])
        copy.start()
        loads.append(copy)
        return copy

    def act_cols(o):
        return pl.ds(pl.multiple_of(z_at(o) * 128, 128), 128)

    z_order = far_first(nz) + [0]
    dy_load = load(dy_hbm, dy)
    act_loads = [load(act_hbm.at[:, act_cols(o)], act.at[i]) for i, o in enumerate(z_order)]
    other_loads = [
        load(left_hbm, left_old),
        load(right_hbm, right_old),
        load(p_left_hbm, p_left),
        load(p_right_hbm, p_right),
    ]

    def slab_rows(z_, xl_):
        return pl.ds(pl.multiple_of((z_ * 2 + xl_) * SLAB, SLAB), SLAB)

    def pair_rows(z_):
        return pl.ds(pl.multiple_of(z_ * 2 * SLAB, 2 * SLAB), 2 * SLAB)

    def half_cols(c_):
        return pl.ds(pl.multiple_of(c_ * HALF, HALF), HALF)

    mine, other = half_cols(c), half_cols(1 - c)

    class Scatter:
        def __init__(self, part, rc, xs, rx, zs, rz):
            self.part, self.rc, self.xs, self.rx, self.zs, self.rz = part, rc, xs, rx, zs, rz
            self.ic = [net.slot() for _ in range(nz)]
            self.ix = [net.slot() for _ in range(nz)]
            self.iz = [net.slot() for _ in range(nz)]

        def block(self, o, value):
            rows = pair_rows(z_at(o))
            self.part[rows, :] = value
            net.send(self.ic[o], self.part.at[rows, other], self.rc.at[rows, :], core_peer)

        def over_x(self, o):
            rows = pair_rows(z_at(o))
            net.arrive(self.ic[o], self.rc.at[rows, :], core_peer)
            theirs = slab_rows(z_at(o), 1 - xl)
            self.xs[o] = self.part[theirs, mine] + self.rc[theirs, :]
            net.send(self.ix[o], self.xs.at[o], self.rx.at[o], x_peer)

        def over_z(self, o):
            net.arrive(self.ix[o], self.rx.at[o], x_peer)
            ours = slab_rows(z_at(o), xl)
            self.zs[o] = self.part[ours, mine] + self.rc[ours, :] + self.rx[o]
            if o:
                net.send(self.iz[o], self.zs.at[o], self.rz.at[o], z_peer(o))

        def total(self):
            value = self.zs[0]
            for o in near_first(nz):
                net.arrive(self.iz[o], self.rz.at[o], z_peer(o))
                value = value + self.rz[o]
            return value

    class Gather:
        def __init__(self, full):
            self.full = full
            self.ic = [net.slot() for _ in range(nz)]
            self.ix = [net.slot() for _ in range(nz)]
            self.iz = [net.slot() for _ in range(nz)]

        def over_z(self, value):
            rows = slab_rows(z, xl)
            self.full[rows, mine] = value
            chunk = self.full.at[rows, mine]
            for o in far_first(nz):
                net.send(self.iz[o], chunk, chunk, z_peer(o))
            net.send(self.ix[0], chunk, chunk, x_peer)

        def over_x(self, o):
            chunk = self.full.at[slab_rows(z_at(nz - o), xl), mine]
            net.arrive(self.iz[o], chunk, z_peer(nz - o))
            net.send(self.ix[o], chunk, chunk, x_peer)

        def over_core(self, o):
            z_ = z_at(nz - o)
            net.arrive(self.ix[o], self.full.at[slab_rows(z_, 1 - xl), mine], x_peer)
            pair = self.full.at[pair_rows(z_), mine]
            net.send(self.ic[o], pair, pair, core_peer)

        def landed(self, o):
            net.arrive(self.ic[o], self.full.at[pair_rows(z_at(nz - o)), other], core_peer)

    class Sum:
        def __init__(self, buf, recv, zrecv):
            self.buf, self.recv, self.zrecv = buf, recv, zrecv
            self.ic, self.ix = net.slot(), net.slot()
            self.iz = [net.slot() for _ in range(nz)]

        def over_core(self):
            net.send(self.ic, self.buf.at[0], self.recv.at[0], core_peer)

        def over_x(self):
            net.arrive(self.ic, self.recv.at[0], core_peer)
            self.buf[1] = self.buf[0] + self.recv[0]
            net.send(self.ix, self.buf.at[1], self.recv.at[1], x_peer)

        def over_z(self):
            net.arrive(self.ix, self.recv.at[1], x_peer)
            self.buf[2] = self.buf[1] + self.recv[1]
            for o in far_first(nz):
                net.send(self.iz[o], self.buf.at[2], self.zrecv.at[o], z_peer(o))

        def total(self):
            value = self.buf[2]
            for o in near_first(nz):
                net.arrive(self.iz[o], self.zrecv.at[o], z_peer(o))
                value = value + self.zrecv[o]
            return value

    class SumA:
        def __init__(self, buf, recv, yrecv):
            self.buf, self.recv, self.yrecv = buf, recv, yrecv
            self.ix = net.slot()
            self.iy = [net.slot() for _ in range(ny)]

        def over_hi(self):
            net.send(self.ix, self.buf.at[0], self.recv, hi_peer)

        def over_y(self):
            net.arrive(self.ix, self.recv, hi_peer)
            self.buf[1] = self.buf[0] + self.recv[...]
            for o in far_first(ny):
                net.send(self.iy[o], self.buf.at[1], self.yrecv.at[o], y_peer(o))

        def total(self):
            value = self.buf[1]
            for o in near_first(ny):
                net.arrive(self.iy[o], self.yrecv.at[o], y_peer(o))
                value = value + self.yrecv[o]
            return value

    old_sum = Sum(abuf, arecv, azrecv)
    h_sum = SumA(hbuf, hrecv, hyrecv)
    image_sum = SumA(bbuf, brecv, byrecv)
    left_sum = Sum(fbuf, frecv, fzrecv)
    last_sum = Sum(cbuf, crecv, czrecv)

    first = Scatter(part, rc, xs, rx, zs, rz)
    gather = Gather(grad)

    def grad_block(i):
        act_loads[i].wait()
        return lax.dot_general(act[i], dy[...], TN, preferred_element_type=F32)

    def blocks_and_x(scatter, block_of, between=()):
        between = dict(between)
        for i in range(nz):
            scatter.block(z_order[i], block_of(i))
            if i in between:
                between[i]()
            if i >= 3:
                scatter.over_x(z_order[i - 3])
        for i in range(nz - 3, nz):
            if i >= 0:
                scatter.over_x(z_order[i])

    dy_load.wait()
    first_value = grad_block(0)
    pl.semaphore_wait(barrier, 5 + (nz - 1) + (ny - 1))
    blocks_and_x(first, lambda i: grad_block(i) if i else first_value)

    for copy in other_loads:
        copy.wait()
    row = lax.broadcasted_iota(jnp.int32, (8, 128), 0)
    p_row = jnp.broadcast_to(p_right[pl.ds(dp, 1), :], (8, 128))
    old_right = dot3(halves(p_row), halves(right_old[...]), NT)
    abuf[0] = jnp.where(row == 0, old_right[:, :HALF], old_right[:, HALF:])
    old_sum.over_core()
    for o in z_order[: nz // 2]:
        first.over_z(o)
    old_sum.over_x()
    for o in z_order[nz // 2 :]:
        first.over_z(o)
    old_sum.over_z()
    gown[...] = first.total()

    i_flip, i_flip_2 = net.slot(), net.slot()
    iy = [net.slot() for _ in range(ny)]
    ih = [net.slot() for _ in range(ny)]

    def panel_z(y_):
        return (z + y_ - b % ny + ny // 2 + nz) % nz

    def panel_slab(mp_, y_):
        return panel.at[slab_rows(panel_z(y_), jnp.where(mp_ == b // ny, xl, 1 - xl)), :]

    chunk = panel.at[slab_rows(z, xl), :]
    net.send(i_flip, gown, chunk, flip_to)
    net.send(i_flip_2, gown, chunk, flip_to_2)
    gather.over_z(gown[...])
    far = [o for o in far_first(ny) if min(o, ny - o) > 2]
    near = [o for o in far_first(ny) if min(o, ny - o) <= 2]
    net.arrive(i_flip, panel_slab(mp, pre), flip_from)
    for o in far:
        net.send(iy[o], panel_slab(mp, pre), panel_slab(mp, pre), y_peer(o))
    net.arrive(i_flip_2, panel_slab(1 - mp, pre), flip_from_2)
    own_pair = panel.at[pair_rows(panel_z(pre)), :]
    for o in near:
        net.send(iy[o], own_pair, own_pair, y_peer(o))
    for o in near_first(nz):
        gather.over_x(o)
    for o in reversed(far):
        slab = panel_slab(mp, y_at(ny - o))
        net.arrive(iy[o], slab, y_peer(ny - o))
        net.send(ih[o], slab, slab, hi_peer)
    for o in [0] + near_first(nz):
        gather.over_core(o)
    for o in [0] + near_first(nz):
        gather.landed(o)

    il = [net.slot() for _ in range(ny)]
    ilx = net.slot()
    ilg = [net.slot() for _ in range(ny)]
    own32 = pl.ds(pl.multiple_of(dp * 32, 32), 32)
    grad_split = halves(grad[...])
    probe_a = jnp.concatenate([p_right[pl.ds(2 * a, 1), :], p_right[pl.ds(2 * a + 1, 1), :]], axis=1)
    rows40 = jnp.concatenate([grad[own32, :], jnp.broadcast_to(probe_a, (8, 2 * HALF))], axis=0)
    both = dot3(halves(rows40), grad_split, NT)
    for j in range(rows_l):
        hbuf[0, pl.ds(j, 1), :] = both[32:33, j * 128 : (j + 1) * 128]
    h_sum.over_hi()
    lpart[...] = both[0:32, :] * (1.0 / ff)
    old_lanes = pl.ds(pl.multiple_of((a // 2) * 128, 128), 128)
    old = left_old[...] * DECAY
    side = lax.broadcasted_iota(jnp.int32, (32, 128), 1) // SLAB
    lpart[:, old_lanes] += jnp.where(side == a % 2, jnp.concatenate([old, old], axis=1), 0.0)

    def l_lanes(y_):
        return pl.ds(pl.multiple_of(y_ * 128, 128), 128)

    for o in far_first(ny):
        net.send(il[o], lpart.at[:, l_lanes(y_at(o))], lr.at[o], y_peer(o))
    for o in near:
        net.arrive(iy[o], panel.at[pair_rows(panel_z(y_at(ny - o))), :], y_peer(ny - o))
    h_sum.over_y()
    for o in reversed(far):
        net.arrive(ih[o], panel_slab(1 - mp, y_at(ny - o)), hi_peer)

    gram = dot3(halves(panel[...].T), grad_split, NN)
    rtile[...] = right_old[...].T * DECAY + gram * (1.0 / d_model)
    rt_split = halves(rtile[...])

    second = Scatter(part2, rc2, xs2, rx2, zs2, rz2)
    gather2 = Gather(prod)

    def prod_block(i):
        return dot3(halves(panel[pair_rows(z_at(z_order[i])), :]), rt_split, NN)

    def right_images():
        h = h_sum.total()
        h_row = jnp.concatenate([h[j : j + 1, :] for j in range(rows_l)], axis=1)
        new = dot3(halves(jnp.broadcast_to(h_row, (8, d_model))), grad_split, NN)
        old_image = old_sum.total()
        f_old = jnp.concatenate([old_image[0:1, :], old_image[1:2, :]], axis=1)
        f_row = f_old * DECAY + new[0:1, :] * (1.0 / d_model)
        square = jnp.sum(f_row * f_row, axis=1, keepdims=True)
        image = dot3(halves(jnp.broadcast_to(f_row, (8, 2 * HALF))), rt_split, NT)
        bbuf[0] = jnp.where(row == 0, image, square)
        image_sum.over_hi()

    def left_rows():
        total = lpart[:, l_lanes(pre)]
        for o in near_first(ny):
            net.arrive(il[o], lr.at[o], y_peer(o))
            total = total + lr[o]
        lsum[...] = total
        net.send(ilx, lsum, lx, hi_peer)

    blocks_and_x(second, prod_block, {min(3, nz - 1): right_images, nz - 1: left_rows})
    image_sum.over_y()
    net.arrive(ilx, lx, hi_peer)
    lrow[:, l_lanes(pre)] = lsum[...] + lx[...]
    own_lanes = lrow.at[:, l_lanes(pre)]
    for o in far_first(ny):
        net.send(ilg[o], own_lanes, own_lanes, y_peer(o))
    for o in z_order:
        second.over_z(o)

    whole = image_sum.total()
    norm_right = jnp.sqrt(whole[1:2, 0:1] + FLOOR)
    scaled = whole[0:1, :] / norm_right
    right_part = jnp.sum(scaled * scaled, axis=1, keepdims=True)
    cbuf[0] = jnp.broadcast_to(right_part, (8, 128))
    last_sum.over_core()

    for o in near_first(ny):
        net.arrive(ilg[o], lrow.at[:, l_lanes(y_at(ny - o))], y_peer(ny - o))
    last_sum.over_x()
    f_left = jnp.zeros((32, 1), F32)
    for j in range(rows_l):
        f_left = f_left + jnp.sum(
            lrow[:, j * 128 : (j + 1) * 128] * p_left[pl.ds(j, 1), :], axis=1, keepdims=True
        )
    left_image = jnp.sum(lrow[...] * f_left, axis=0, keepdims=True)
    for j in range(rows_l):
        fbuf[0, pl.ds(j, 1), :] = left_image[:, j * 128 : (j + 1) * 128]
    left_square = jnp.sum(f_left * f_left, axis=0, keepdims=True)
    fbuf[0, pl.ds(rows_l, 8), :] = jnp.broadcast_to(left_square, (8, 128))
    left_sum.over_core()
    last_sum.over_z()
    left_sum.over_x()

    gather2.over_z(second.total())
    left_sum.over_z()

    left_grad = dot3(halves(lrow[...]), grad_split, NN)
    right_out[...] = rtile[...].T
    lanes = lrow[:, old_lanes]
    left_out[...] = jnp.where(a % 2 == 0, lanes[:, :SLAB], lanes[:, SLAB:])
    for o in near_first(nz):
        gather2.over_x(o)
    for o in [0] + near_first(nz):
        gather2.over_core(o)
    top_right = jnp.sqrt(last_sum.total()[0:1, 0:1] + FLOOR)
    images = left_sum.total()
    norm_left = jnp.sqrt(images[rows_l : rows_l + 1, 0:1] + FLOOR)
    unit_image = images[0:rows_l, :] / norm_left
    top_left = jnp.sqrt(
        jnp.sum(jnp.sum(unit_image * unit_image, axis=1, keepdims=True), axis=0, keepdims=True)
        + FLOOR
    )
    scale = lax.rsqrt(jnp.sqrt(top_left * top_right)) * 0.0625
    left_prod = jnp.zeros_like(left_grad)
    for o in [0] + near_first(nz):
        gather2.landed(o)
        z_ = z_at(nz - o)
        left_prod = left_prod + dot3(
            halves(lrow[:, l_lanes(z_)]), halves(prod[pair_rows(z_), :]), NN
        )
    own = 5.0 * grad[own32, :] - prod[own32, :] / top_right
    left_term = 5.0 * left_grad - left_prod / top_right
    update_out[...] = (5.0 * own - left_term / top_left) * scale

    net.finish()


def store(left, right, update, left_out, right_out, update_out, sem):
    pairs = ((left, left_out), (right, right_out), (update, update_out))
    copies = [pltpu.make_async_copy(src, dst, sem.at[i]) for i, (src, dst) in enumerate(pairs)]
    for copy in copies:
        copy.start()
    for copy in copies:
        copy.wait()


def step(nz, ny, ff, activations, grad_output, left_old, right_old, probe_left, probe_right):
    d_model = activations.shape[1]
    block = grad_output.shape[1]
    rows_l = d_model // 128
    vmem = pltpu.VMEM

    def scatter_bufs():
        return [
            vmem((d_model, block), F32),
            vmem((d_model, HALF), F32),
            vmem((nz, SLAB, HALF), F32),
            vmem((nz, SLAB, HALF), F32),
            vmem((nz, SLAB, HALF), F32),
            vmem((nz, SLAB, HALF), F32),
            vmem((d_model, block), F32),
        ]

    scratch = [
        vmem((nz, activations.shape[0], 128), BF16),
        vmem(grad_output.shape, BF16),
        vmem((left_old.shape[1], left_old.shape[0]), F32),
        vmem(right_old.shape, F32),
        vmem((probe_left.shape[0] // 128, 128), F32),
        vmem((probe_right.shape[0] // 128, 128), F32),
        *scatter_bufs(),
        *scatter_bufs(),
        vmem((SLAB, HALF), F32),
        vmem((d_model, HALF), F32),
        vmem((HALF, block), F32),
        vmem((32, d_model), F32),
        vmem((ny, 32, 128), F32),
        vmem((32, 128), F32),
        vmem((32, 128), F32),
        vmem((32, d_model), F32),
        vmem((3, 8, 128), F32),
        vmem((2, 8, 128), F32),
        vmem((nz, 8, 128), F32),
        vmem((2, rows_l, 128), F32),
        vmem((rows_l, 128), F32),
        vmem((ny, rows_l, 128), F32),
        vmem((3, rows_l + 8, 128), F32),
        vmem((2, rows_l + 8, 128), F32),
        vmem((nz, rows_l + 8, 128), F32),
        vmem((2, 8, 128), F32),
        vmem((8, 128), F32),
        vmem((ny, 8, 128), F32),
        vmem((3, 8, 128), F32),
        vmem((2, 8, 128), F32),
        vmem((nz, 8, 128), F32),
        pltpu.SemaphoreType.DMA((COPIES,)),
        pltpu.SemaphoreType.DMA((COPIES,)),
        pltpu.SemaphoreType.DMA((nz + 5,)),
    ]
    spec = pl.BlockSpec(memory_space=pltpu.VMEM)
    left, right, update = pl.pallas_call(
        functools.partial(kernel, nz, ny, ff),
        out_shape=(
            jax.ShapeDtypeStruct((left_old.shape[1], left_old.shape[0]), F32),
            jax.ShapeDtypeStruct(right_old.shape, F32),
            jax.ShapeDtypeStruct((d_model // (4 * nz), block), F32),
        ),
        in_specs=[pl.BlockSpec(memory_space=pltpu.HBM)] * 6,
        out_specs=(spec,) * 3,
        scratch_shapes=scratch,
        compiler_params=pltpu.CompilerParams(
            collective_id=0, has_side_effects=True, vmem_limit_bytes=58 * 1024 * 1024
        ),
        name="shampoo",
    )(
        activations,
        grad_output,
        left_old.T,
        right_old,
        probe_left.reshape(-1, 128),
        probe_right.reshape(-1, 128),
    )
    left, right, update = pl.pallas_call(
        store,
        out_shape=tuple(jax.ShapeDtypeStruct(r.shape, F32) for r in (left, right, update)),
        in_specs=[spec] * 3,
        out_specs=(pl.BlockSpec(memory_space=pltpu.HBM),) * 3,
        scratch_shapes=[pltpu.SemaphoreType.DMA((3,))],
        name="store",
    )(left, right, update)
    return left.T, right, update


def solution(mesh):
    nz = mesh.shape["dp"] // 4
    ny = mesh.shape["pre"]
    in_specs = (
        P("dp", None),
        P("dp", ("mp", "pre")),
        P(("mp", "pre"), "dp"),
        P(("mp", "pre"), "dp"),
        P(),
        P(),
    )
    out_specs = (P(("mp", "pre"), "dp"), P(("mp", "pre"), "dp"), P("dp", ("mp", "pre")))
    ff = 2 * ny * 2 * HALF
    return jax.shard_map(
        functools.partial(step, nz, ny, ff),
        mesh=mesh,
        in_specs=in_specs,
        out_specs=out_specs,
        check_vma=False,
    )
```

```python
import functools

import jax
import jax.numpy as jnp
from jax import lax
from jax.experimental import pallas as pl
from jax.experimental.pallas import tpu as pltpu
from jax.sharding import PartitionSpec as P

MESH = pl.DeviceIdType.MESH
F32 = jnp.float32
BF16 = jnp.bfloat16

DECAY = 0.9
FLOOR = 1e-06
SLAB = 64
HALF = 128
COPIES = 216

NN = (((1,), (0,)), ((), ()))
NT = (((1,), (1,)), ((), ()))
TN = (((0,), (0,)), ((), ()))


def far_first(n):
    return sorted(range(1, n), key=lambda o: -min(o, n - o))


def near_first(n):
    return sorted(range(1, n), key=lambda o: min(o, n - o))


def halves(v):
    high = v.astype(BF16)
    return high, (v - high.astype(F32)).astype(BF16)


def dot3(a, b, dims):
    (ah, al), (bh, bl) = a, b
    dot = functools.partial(lax.dot_general, dimension_numbers=dims, preferred_element_type=F32)
    return dot(ah, bh) + (dot(ah, bl) + dot(al, bh))


class Net:
    def __init__(self, send_sem, recv_sem):
        self.send_sem, self.recv_sem, self.used, self.sent = send_sem, recv_sem, 0, []

    def slot(self):
        self.used += 1
        assert self.used <= COPIES
        return self.used - 1

    def copy(self, i, src, dst, device):
        return pltpu.make_async_remote_copy(
            src_ref=src,
            dst_ref=dst,
            send_sem=self.send_sem.at[i],
            recv_sem=self.recv_sem.at[i],
            device_id=device,
            device_id_type=MESH,
        )

    def send(self, i, src, dst, device):
        copy = self.copy(i, src, dst, device)
        copy.start()
        self.sent.append(copy)

    def arrive(self, i, dst, device):
        self.copy(i, dst, dst, device).wait_recv()

    def finish(self):
        for copy in self.sent:
            copy.wait_send()


def kernel(
    nz,
    ny,
    ff,
    act_hbm,
    dy_hbm,
    left_hbm,
    right_hbm,
    p_left_hbm,
    p_right_hbm,
    left_out,
    right_out,
    update_out,
    act,
    dy,
    left_old,
    right_old,
    p_left,
    p_right,
    part,
    rc,
    xs,
    rx,
    zs,
    rz,
    grad,
    part2,
    rc2,
    xs2,
    rx2,
    zs2,
    rz2,
    prod,
    gown,
    panel,
    rtile,
    lpart,
    lr,
    lsum,
    lx,
    lrow,
    abuf,
    arecv,
    azrecv,
    hbuf,
    hrecv,
    hyrecv,
    fbuf,
    frecv,
    fzrecv,
    bbuf,
    brecv,
    byrecv,
    cbuf,
    crecv,
    czrecv,
    send_sem,
    recv_sem,
    load_sem,
):
    d_model = nz * 2 * SLAB
    rows_l = d_model // 128
    dp, mp, pre = lax.axis_index("dp"), lax.axis_index("mp"), lax.axis_index("pre")
    z, xl, c = dp // 4, (dp // 2) % 2, dp % 2
    a = mp * ny + pre
    b = z * 2 + xl
    core_peer = (dp + 1 - 2 * c, mp, pre)
    x_peer = (dp + 2 - 4 * xl, mp, pre)
    hi_peer = (dp, 1 - mp, pre)

    turn = (z - a // 2 + ny // 2 + nz) % nz
    goal_hi = jnp.where(xl == a % 2, mp, 1 - mp)
    flip_to = (a * 2 + c, goal_hi, (pre + turn) % ny)
    came = (z + pre - b % ny + ny // 2 + nz) % nz
    came_lo = jnp.where(mp == b // ny, xl, 1 - xl)
    flip_from = (came * 4 + came_lo * 2 + c, b // ny, b % ny)
    flip_to_2 = (a * 2 + c, 1 - goal_hi, (pre + turn) % ny)
    flip_from_2 = (came * 4 + (1 - came_lo) * 2 + c, b // ny, b % ny)

    def z_at(o):
        return (z + o) % nz

    def z_peer(o):
        return (z_at(o) * 4 + xl * 2 + c, mp, pre)

    def y_at(o):
        return (pre + o) % ny

    def y_peer(o):
        return (dp, mp, y_at(o))

    net = Net(send_sem, recv_sem)

    barrier = pltpu.get_barrier_semaphore()

    def greet(device):
        pl.semaphore_signal(barrier, inc=1, device_id=device, device_id_type=MESH)

    loads = []

    def load(src, dst):
        copy = pltpu.make_async_copy(src, dst, load_sem.at[len(loads)])
        copy.start()
        loads.append(copy)
        return copy

    def act_cols(o):
        return pl.ds(pl.multiple_of(z_at(o) * 128, 128), 128)

    z_order = far_first(nz) + [0]
    dy_load = load(dy_hbm, dy)
    act_loads = [load(act_hbm.at[:, act_cols(o)], act.at[i]) for i, o in enumerate(z_order)]
    other_loads = [
        load(left_hbm, left_old),
        load(right_hbm, right_old),
        load(p_left_hbm, p_left),
        load(p_right_hbm, p_right),
    ]

    greet(core_peer)
    greet(x_peer)
    greet(hi_peer)
    for o in range(1, nz):
        greet(z_peer(o))
    for o in range(1, ny):
        greet(y_peer(o))

    greet(flip_from)
    greet(flip_from_2)

    def slab_rows(z_, xl_):
        return pl.ds(pl.multiple_of((z_ * 2 + xl_) * SLAB, SLAB), SLAB)

    def pair_rows(z_):
        return pl.ds(pl.multiple_of(z_ * 2 * SLAB, 2 * SLAB), 2 * SLAB)

    def half_cols(c_):
        return pl.ds(pl.multiple_of(c_ * HALF, HALF), HALF)

    mine, other = half_cols(c), half_cols(1 - c)

    class Scatter:
        def __init__(self, part, rc, xs, rx, zs, rz):
            self.part, self.rc, self.xs, self.rx, self.zs, self.rz = part, rc, xs, rx, zs, rz
            self.ic = [net.slot() for _ in range(nz)]
            self.ix = [net.slot() for _ in range(nz)]
            self.iz = [net.slot() for _ in range(nz)]

        def block(self, o, value):
            rows = pair_rows(z_at(o))
            self.part[rows, :] = value
            net.send(self.ic[o], self.part.at[rows, other], self.rc.at[rows, :], core_peer)

        def over_x(self, o):
            rows = pair_rows(z_at(o))
            net.arrive(self.ic[o], self.rc.at[rows, :], core_peer)
            theirs = slab_rows(z_at(o), 1 - xl)
            self.xs[o] = self.part[theirs, mine] + self.rc[theirs, :]
            net.send(self.ix[o], self.xs.at[o], self.rx.at[o], x_peer)

        def over_z(self, o):
            net.arrive(self.ix[o], self.rx.at[o], x_peer)
            ours = slab_rows(z_at(o), xl)
            self.zs[o] = self.part[ours, mine] + self.rc[ours, :] + self.rx[o]
            if o:
                net.send(self.iz[o], self.zs.at[o], self.rz.at[o], z_peer(o))

        def total(self):
            value = self.zs[0]
            for o in near_first(nz):
                net.arrive(self.iz[o], self.rz.at[o], z_peer(o))
                value = value + self.rz[o]
            return value

    class Gather:
        def __init__(self, full):
            self.full = full
            self.ic = [net.slot() for _ in range(nz)]
            self.ix = [net.slot() for _ in range(nz)]
            self.iz = [net.slot() for _ in range(nz)]

        def over_z(self, value):
            rows = slab_rows(z, xl)
            self.full[rows, mine] = value
            chunk = self.full.at[rows, mine]
            net.send(self.ix[0], chunk, chunk, x_peer)
            for o in near_first(nz):
                net.send(self.iz[o], chunk, chunk, z_peer(o))

        def over_x(self, o):
            chunk = self.full.at[slab_rows(z_at(nz - o), xl), mine]
            net.arrive(self.iz[o], chunk, z_peer(nz - o))
            net.send(self.ix[o], chunk, chunk, x_peer)

        def over_core(self, o):
            z_ = z_at(nz - o)
            net.arrive(self.ix[o], self.full.at[slab_rows(z_, 1 - xl), mine], x_peer)
            pair = self.full.at[pair_rows(z_), mine]
            net.send(self.ic[o], pair, pair, core_peer)

        def landed(self, o):
            net.arrive(self.ic[o], self.full.at[pair_rows(z_at(nz - o)), other], core_peer)

    class Sum:
        def __init__(self, buf, recv, zrecv):
            self.buf, self.recv, self.zrecv = buf, recv, zrecv
            self.ic, self.ix = net.slot(), net.slot()
            self.iz = [net.slot() for _ in range(nz)]

        def over_core(self):
            net.send(self.ic, self.buf.at[0], self.recv.at[0], core_peer)

        def over_x(self):
            net.arrive(self.ic, self.recv.at[0], core_peer)
            self.buf[1] = self.buf[0] + self.recv[0]
            net.send(self.ix, self.buf.at[1], self.recv.at[1], x_peer)

        def over_z(self):
            net.arrive(self.ix, self.recv.at[1], x_peer)
            self.buf[2] = self.buf[1] + self.recv[1]
            for o in far_first(nz):
                net.send(self.iz[o], self.buf.at[2], self.zrecv.at[o], z_peer(o))

        def total(self):
            value = self.buf[2]
            for o in near_first(nz):
                net.arrive(self.iz[o], self.zrecv.at[o], z_peer(o))
                value = value + self.zrecv[o]
            return value

    class SumA:
        def __init__(self, buf, recv, yrecv):
            self.buf, self.recv, self.yrecv = buf, recv, yrecv
            self.ix = net.slot()
            self.iy = [net.slot() for _ in range(ny)]

        def over_hi(self):
            net.send(self.ix, self.buf.at[0], self.recv, hi_peer)

        def over_y(self):
            net.arrive(self.ix, self.recv, hi_peer)
            self.buf[1] = self.buf[0] + self.recv[...]
            for o in far_first(ny):
                net.send(self.iy[o], self.buf.at[1], self.yrecv.at[o], y_peer(o))

        def total(self):
            value = self.buf[1]
            for o in near_first(ny):
                net.arrive(self.iy[o], self.yrecv.at[o], y_peer(o))
                value = value + self.yrecv[o]
            return value

    old_sum = Sum(abuf, arecv, azrecv)
    h_sum = SumA(hbuf, hrecv, hyrecv)
    image_sum = SumA(bbuf, brecv, byrecv)
    left_sum = Sum(fbuf, frecv, fzrecv)
    last_sum = Sum(cbuf, crecv, czrecv)

    first = Scatter(part, rc, xs, rx, zs, rz)
    gather = Gather(grad)

    def grad_block(i):
        act_loads[i].wait()
        return lax.dot_general(act[i], dy[...], TN, preferred_element_type=F32)

    def blocks_and_x(scatter, block_of, between=()):
        between = dict(between)
        for i in range(nz):
            scatter.block(z_order[i], block_of(i))
            if i in between:
                between[i]()
            if i >= 3:
                scatter.over_x(z_order[i - 3])
        for i in range(nz - 3, nz):
            if i >= 0:
                scatter.over_x(z_order[i])

    dy_load.wait()
    first_value = grad_block(0)
    pl.semaphore_wait(barrier, 5 + (nz - 1) + (ny - 1))
    blocks_and_x(first, lambda i: grad_block(i) if i else first_value)

    for copy in other_loads:
        copy.wait()
    row = lax.broadcasted_iota(jnp.int32, (8, 128), 0)
    p_row = jnp.broadcast_to(p_right[pl.ds(dp, 1), :], (8, 128))
    old_right = dot3(halves(p_row), halves(right_old[...]), NT)
    abuf[0] = jnp.where(row == 0, old_right[:, :HALF], old_right[:, HALF:])
    old_sum.over_core()
    for o in z_order[: nz // 2]:
        first.over_z(o)
    old_sum.over_x()
    for o in z_order[nz // 2 :]:
        first.over_z(o)
    old_sum.over_z()
    gown[...] = first.total()

    i_flip, i_flip_2 = net.slot(), net.slot()
    iy = [net.slot() for _ in range(ny)]
    ih = [net.slot() for _ in range(ny)]

    def panel_z(y_):
        return (z + y_ - b % ny + ny // 2 + nz) % nz

    def panel_slab(mp_, y_):
        return panel.at[slab_rows(panel_z(y_), jnp.where(mp_ == b // ny, xl, 1 - xl)), :]

    chunk = panel.at[slab_rows(z, xl), :]
    net.send(i_flip, gown, chunk, flip_to)
    net.send(i_flip_2, gown, chunk, flip_to_2)
    gather.over_z(gown[...])
    far = [o for o in far_first(ny) if min(o, ny - o) > 2]
    near = [o for o in far_first(ny) if min(o, ny - o) <= 2]
    net.arrive(i_flip, panel_slab(mp, pre), flip_from)
    for o in far:
        net.send(iy[o], panel_slab(mp, pre), panel_slab(mp, pre), y_peer(o))
    net.arrive(i_flip_2, panel_slab(1 - mp, pre), flip_from_2)
    own_pair = panel.at[pair_rows(panel_z(pre)), :]
    for o in near:
        net.send(iy[o], own_pair, own_pair, y_peer(o))
    for o in near_first(nz):
        gather.over_x(o)
    core_order = [0] + near_first(nz)
    for o in core_order[: nz // 2 + 1]:
        gather.over_core(o)
    for o in reversed(far):
        slab = panel_slab(mp, y_at(ny - o))
        net.arrive(iy[o], slab, y_peer(ny - o))
        net.send(ih[o], slab, slab, hi_peer)
    for o in core_order[nz // 2 + 1 :]:
        gather.over_core(o)
    for o in [0] + near_first(nz):
        gather.landed(o)

    il = [net.slot() for _ in range(ny)]
    ilx = net.slot()
    ilg = [net.slot() for _ in range(ny)]
    own32 = pl.ds(pl.multiple_of(dp * 32, 32), 32)
    grad_split = halves(grad[...])
    probe_a = jnp.concatenate([p_right[pl.ds(2 * a, 1), :], p_right[pl.ds(2 * a + 1, 1), :]], axis=1)
    rows40 = jnp.concatenate([grad[own32, :], jnp.broadcast_to(probe_a, (8, 2 * HALF))], axis=0)
    both = dot3(halves(rows40), grad_split, NT)
    for j in range(rows_l):
        hbuf[0, pl.ds(j, 1), :] = both[32:33, j * 128 : (j + 1) * 128]
    h_sum.over_hi()
    lpart[...] = both[0:32, :] * (1.0 / ff)
    old_lanes = pl.ds(pl.multiple_of((a // 2) * 128, 128), 128)
    old = left_old[...] * DECAY
    side = lax.broadcasted_iota(jnp.int32, (32, 128), 1) // SLAB
    lpart[:, old_lanes] += jnp.where(side == a % 2, jnp.concatenate([old, old], axis=1), 0.0)

    def l_lanes(y_):
        return pl.ds(pl.multiple_of(y_ * 128, 128), 128)

    for o in far_first(ny):
        net.send(il[o], lpart.at[:, l_lanes(y_at(o))], lr.at[o], y_peer(o))
    for o in near:
        net.arrive(iy[o], panel.at[pair_rows(panel_z(y_at(ny - o))), :], y_peer(ny - o))
    for o in reversed(far):
        net.arrive(ih[o], panel_slab(1 - mp, y_at(ny - o)), hi_peer)

    gram = dot3(halves(panel[...].T), grad_split, NN)
    rtile[...] = right_old[...].T * DECAY + gram * (1.0 / d_model)
    rt_split = halves(rtile[...])
    h_sum.over_y()

    second = Scatter(part2, rc2, xs2, rx2, zs2, rz2)
    gather2 = Gather(prod)

    def prod_block(i):
        return dot3(halves(panel[pair_rows(z_at(z_order[i])), :]), rt_split, NN)

    def right_images():
        h = h_sum.total()
        h_row = jnp.concatenate([h[j : j + 1, :] for j in range(rows_l)], axis=1)
        new = dot3(halves(jnp.broadcast_to(h_row, (8, d_model))), grad_split, NN)
        old_image = old_sum.total()
        f_old = jnp.concatenate([old_image[0:1, :], old_image[1:2, :]], axis=1)
        f_row = f_old * DECAY + new[0:1, :] * (1.0 / d_model)
        square = jnp.sum(f_row * f_row, axis=1, keepdims=True)
        image = dot3(halves(jnp.broadcast_to(f_row, (8, 2 * HALF))), rt_split, NT)
        bbuf[0] = jnp.where(row == 0, image, square)
        image_sum.over_hi()

    def left_rows():
        total = lpart[:, l_lanes(pre)]
        for o in near_first(ny):
            net.arrive(il[o], lr.at[o], y_peer(o))
            total = total + lr[o]
        lsum[...] = total
        net.send(ilx, lsum, lx, hi_peer)

    blocks_and_x(second, prod_block)
    left_rows()
    cut = [1, 3, 6] if nz > 6 else [1, 1, 1]
    for o in z_order[: cut[0]]:
        second.over_z(o)
    right_images()
    for o in z_order[cut[0] : cut[1]]:
        second.over_z(o)
    net.arrive(ilx, lx, hi_peer)
    lrow[:, l_lanes(pre)] = lsum[...] + lx[...]
    own_lanes = lrow.at[:, l_lanes(pre)]
    for o in far_first(ny):
        net.send(ilg[o], own_lanes, own_lanes, y_peer(o))
    for o in z_order[cut[1] : cut[2]]:
        second.over_z(o)
    image_sum.over_y()
    for o in z_order[cut[2] :]:
        second.over_z(o)

    for o in near_first(ny):
        net.arrive(ilg[o], lrow.at[:, l_lanes(y_at(ny - o))], y_peer(ny - o))
    f_left = jnp.zeros((32, 1), F32)
    for j in range(rows_l):
        f_left = f_left + jnp.sum(
            lrow[:, j * 128 : (j + 1) * 128] * p_left[pl.ds(j, 1), :], axis=1, keepdims=True
        )
    left_image = jnp.sum(lrow[...] * f_left, axis=0, keepdims=True)
    for j in range(rows_l):
        fbuf[0, pl.ds(j, 1), :] = left_image[:, j * 128 : (j + 1) * 128]
    left_square = jnp.sum(f_left * f_left, axis=0, keepdims=True)
    fbuf[0, pl.ds(rows_l, 8), :] = jnp.broadcast_to(left_square, (8, 128))
    left_sum.over_core()

    gather2.over_z(second.total())
    left_sum.over_x()

    whole = image_sum.total()
    norm_right = jnp.sqrt(whole[1:2, 0:1] + FLOOR)
    scaled = whole[0:1, :] / norm_right
    right_part = jnp.sum(scaled * scaled, axis=1, keepdims=True)
    cbuf[0] = jnp.broadcast_to(right_part, (8, 128))
    last_sum.over_core()

    left_grad = dot3(halves(lrow[...]), grad_split, NN)
    right_out[...] = rtile[...].T
    lanes = lrow[:, old_lanes]
    left_out[...] = jnp.where(a % 2 == 0, lanes[:, :SLAB], lanes[:, SLAB:])
    last_sum.over_x()
    left_sum.over_z()
    for o in near_first(nz)[:2]:
        gather2.over_x(o)
    last_sum.over_z()
    for o in near_first(nz)[2:]:
        gather2.over_x(o)
    for o in [0] + near_first(nz):
        gather2.over_core(o)
    top_right = jnp.sqrt(last_sum.total()[0:1, 0:1] + FLOOR)
    images = left_sum.total()
    norm_left = jnp.sqrt(images[rows_l : rows_l + 1, 0:1] + FLOOR)
    unit_image = images[0:rows_l, :] / norm_left
    top_left = jnp.sqrt(
        jnp.sum(jnp.sum(unit_image * unit_image, axis=1, keepdims=True), axis=0, keepdims=True)
        + FLOOR
    )
    scale = lax.rsqrt(jnp.sqrt(top_left * top_right)) * 0.0625
    left_prod = jnp.zeros_like(left_grad)
    for o in [0] + near_first(nz):
        gather2.landed(o)
        z_ = z_at(nz - o)
        left_prod = left_prod + dot3(
            halves(lrow[:, l_lanes(z_)]), halves(prod[pair_rows(z_), :]), NN
        )
    own = 5.0 * grad[own32, :] - prod[own32, :] / top_right
    left_term = 5.0 * left_grad - left_prod / top_right
    update_out[...] = (5.0 * own - left_term / top_left) * scale

    net.finish()


def store(left, right, update, left_out, right_out, update_out, sem):
    pairs = ((left, left_out), (right, right_out), (update, update_out))
    copies = [pltpu.make_async_copy(src, dst, sem.at[i]) for i, (src, dst) in enumerate(pairs)]
    for copy in copies:
        copy.start()
    for copy in copies:
        copy.wait()


def step(nz, ny, ff, activations, grad_output, left_old, right_old, probe_left, probe_right):
    d_model = activations.shape[1]
    block = grad_output.shape[1]
    rows_l = d_model // 128
    vmem = pltpu.VMEM

    def scatter_bufs():
        return [
            vmem((d_model, block), F32),
            vmem((d_model, HALF), F32),
            vmem((nz, SLAB, HALF), F32),
            vmem((nz, SLAB, HALF), F32),
            vmem((nz, SLAB, HALF), F32),
            vmem((nz, SLAB, HALF), F32),
            vmem((d_model, block), F32),
        ]

    scratch = [
        vmem((nz, activations.shape[0], 128), BF16),
        vmem(grad_output.shape, BF16),
        vmem((left_old.shape[1], left_old.shape[0]), F32),
        vmem(right_old.shape, F32),
        vmem((probe_left.shape[0] // 128, 128), F32),
        vmem((probe_right.shape[0] // 128, 128), F32),
        *scatter_bufs(),
        *scatter_bufs(),
        vmem((SLAB, HALF), F32),
        vmem((d_model, HALF), F32),
        vmem((HALF, block), F32),
        vmem((32, d_model), F32),
        vmem((ny, 32, 128), F32),
        vmem((32, 128), F32),
        vmem((32, 128), F32),
        vmem((32, d_model), F32),
        vmem((3, 8, 128), F32),
        vmem((2, 8, 128), F32),
        vmem((nz, 8, 128), F32),
        vmem((2, rows_l, 128), F32),
        vmem((rows_l, 128), F32),
        vmem((ny, rows_l, 128), F32),
        vmem((3, rows_l + 8, 128), F32),
        vmem((2, rows_l + 8, 128), F32),
        vmem((nz, rows_l + 8, 128), F32),
        vmem((2, 8, 128), F32),
        vmem((8, 128), F32),
        vmem((ny, 8, 128), F32),
        vmem((3, 8, 128), F32),
        vmem((2, 8, 128), F32),
        vmem((nz, 8, 128), F32),
        pltpu.SemaphoreType.DMA((COPIES,)),
        pltpu.SemaphoreType.DMA((COPIES,)),
        pltpu.SemaphoreType.DMA((nz + 5,)),
    ]
    spec = pl.BlockSpec(memory_space=pltpu.VMEM)
    left, right, update = pl.pallas_call(
        functools.partial(kernel, nz, ny, ff),
        out_shape=(
            jax.ShapeDtypeStruct((left_old.shape[1], left_old.shape[0]), F32),
            jax.ShapeDtypeStruct(right_old.shape, F32),
            jax.ShapeDtypeStruct((d_model // (4 * nz), block), F32),
        ),
        in_specs=[pl.BlockSpec(memory_space=pltpu.HBM)] * 6,
        out_specs=(spec,) * 3,
        scratch_shapes=scratch,
        compiler_params=pltpu.CompilerParams(
            collective_id=0, has_side_effects=True, vmem_limit_bytes=58 * 1024 * 1024
        ),
        name="shampoo",
    )(
        activations,
        grad_output,
        left_old.T,
        right_old,
        probe_left.reshape(-1, 128),
        probe_right.reshape(-1, 128),
    )
    left, right, update = pl.pallas_call(
        store,
        out_shape=tuple(jax.ShapeDtypeStruct(r.shape, F32) for r in (left, right, update)),
        in_specs=[spec] * 3,
        out_specs=(pl.BlockSpec(memory_space=pltpu.HBM),) * 3,
        scratch_shapes=[pltpu.SemaphoreType.DMA((3,))],
        name="store",
    )(left, right, update)
    return left.T, right, update


def solution(mesh):
    nz = mesh.shape["dp"] // 4
    ny = mesh.shape["pre"]
    in_specs = (
        P("dp", None),
        P("dp", ("mp", "pre")),
        P(("mp", "pre"), "dp"),
        P(("mp", "pre"), "dp"),
        P(),
        P(),
    )
    out_specs = (P(("mp", "pre"), "dp"), P(("mp", "pre"), "dp"), P("dp", ("mp", "pre")))
    ff = 2 * ny * 2 * HALF
    return jax.shard_map(
        functools.partial(step, nz, ny, ff),
        mesh=mesh,
        in_specs=in_specs,
        out_specs=out_specs,
        check_vma=False,
    )
```

```python
import functools

import jax
import jax.numpy as jnp
from jax import lax
from jax.experimental import pallas as pl
from jax.experimental.pallas import tpu as pltpu
from jax.sharding import PartitionSpec as P

MESH = pl.DeviceIdType.MESH
F32 = jnp.float32
BF16 = jnp.bfloat16

DECAY = 0.9
FLOOR = 1e-06
SLAB = 64
HALF = 128
COPIES = 216

NN = (((1,), (0,)), ((), ()))
NT = (((1,), (1,)), ((), ()))
TN = (((0,), (0,)), ((), ()))


def far_first(n):
    return sorted(range(1, n), key=lambda o: -min(o, n - o))


def near_first(n):
    return sorted(range(1, n), key=lambda o: min(o, n - o))


def halves(v):
    high = v.astype(BF16)
    return high, (v - high.astype(F32)).astype(BF16)


def dot3(a, b, dims):
    (ah, al), (bh, bl) = a, b
    dot = functools.partial(lax.dot_general, dimension_numbers=dims, preferred_element_type=F32)
    return dot(ah, bh) + (dot(ah, bl) + dot(al, bh))


class Net:
    def __init__(self, send_sem, recv_sem):
        self.send_sem, self.recv_sem, self.used, self.sent = send_sem, recv_sem, 0, []

    def slot(self):
        self.used += 1
        assert self.used <= COPIES
        return self.used - 1

    def copy(self, i, src, dst, device):
        return pltpu.make_async_remote_copy(
            src_ref=src,
            dst_ref=dst,
            send_sem=self.send_sem.at[i],
            recv_sem=self.recv_sem.at[i],
            device_id=device,
            device_id_type=MESH,
        )

    def send(self, i, src, dst, device):
        copy = self.copy(i, src, dst, device)
        copy.start()
        self.sent.append(copy)

    def arrive(self, i, dst, device):
        self.copy(i, dst, dst, device).wait_recv()

    def finish(self):
        for copy in self.sent:
            copy.wait_send()


def kernel(
    nz,
    ny,
    ff,
    act_hbm,
    dy_hbm,
    left_hbm,
    right_hbm,
    p_left_hbm,
    p_right_hbm,
    left_out,
    right_out,
    update_out,
    act,
    dy,
    left_old,
    right_old,
    p_left,
    p_right,
    part,
    rc,
    xs,
    rx,
    zs,
    rz,
    grad,
    part2,
    rc2,
    xs2,
    rx2,
    zs2,
    rz2,
    prod,
    gown,
    panel,
    rtile,
    lpart,
    lr,
    lsum,
    lx,
    lrow,
    lrows,
    terms,
    xterm,
    sums,
    cterm,
    wrow,
    abuf,
    arecv,
    azrecv,
    hbuf,
    hrecv,
    hyrecv,
    fbuf,
    frecv,
    fzrecv,
    bbuf,
    brecv,
    byrecv,
    cbuf,
    crecv,
    czrecv,
    send_sem,
    recv_sem,
    load_sem,
):
    d_model = nz * 2 * SLAB
    rows_l = d_model // 128
    dp, mp, pre = lax.axis_index("dp"), lax.axis_index("mp"), lax.axis_index("pre")
    z, xl, c = dp // 4, (dp // 2) % 2, dp % 2
    a = mp * ny + pre
    b = z * 2 + xl
    core_peer = (dp + 1 - 2 * c, mp, pre)
    x_peer = (dp + 2 - 4 * xl, mp, pre)
    hi_peer = (dp, 1 - mp, pre)

    turn = (z - a // 2 + ny // 2 + nz) % nz
    goal_hi = jnp.where(xl == a % 2, mp, 1 - mp)
    flip_to = (a * 2 + c, goal_hi, (pre + turn) % ny)
    came = (z + pre - b % ny + ny // 2 + nz) % nz
    came_lo = jnp.where(mp == b // ny, xl, 1 - xl)
    flip_from = (came * 4 + came_lo * 2 + c, b // ny, b % ny)
    flip_to_2 = (a * 2 + c, 1 - goal_hi, (pre + turn) % ny)
    flip_from_2 = (came * 4 + (1 - came_lo) * 2 + c, b // ny, b % ny)

    def z_at(o):
        return (z + o) % nz

    def z_peer(o):
        return (z_at(o) * 4 + xl * 2 + c, mp, pre)

    def y_at(o):
        return (pre + o) % ny

    def y_peer(o):
        return (dp, mp, y_at(o))

    net = Net(send_sem, recv_sem)

    barrier = pltpu.get_barrier_semaphore()

    def greet(device):
        pl.semaphore_signal(barrier, inc=1, device_id=device, device_id_type=MESH)

    loads = []

    def load(src, dst):
        copy = pltpu.make_async_copy(src, dst, load_sem.at[len(loads)])
        copy.start()
        loads.append(copy)
        return copy

    def act_cols(o):
        return pl.ds(pl.multiple_of(z_at(o) * 128, 128), 128)

    z_order = far_first(nz) + [0]
    dy_load = load(dy_hbm, dy)
    act_loads = [load(act_hbm.at[:, act_cols(o)], act.at[i]) for i, o in enumerate(z_order)]
    other_loads = [
        load(left_hbm, left_old),
        load(right_hbm, right_old),
        load(p_left_hbm, p_left),
        load(p_right_hbm, p_right),
    ]

    greet(core_peer)
    greet(x_peer)
    greet(hi_peer)
    for o in range(1, nz):
        greet(z_peer(o))
    for o in range(1, ny):
        greet(y_peer(o))

    greet(flip_from)
    greet(flip_from_2)

    def slab_rows(z_, xl_):
        return pl.ds(pl.multiple_of((z_ * 2 + xl_) * SLAB, SLAB), SLAB)

    def pair_rows(z_):
        return pl.ds(pl.multiple_of(z_ * 2 * SLAB, 2 * SLAB), 2 * SLAB)

    def half_cols(c_):
        return pl.ds(pl.multiple_of(c_ * HALF, HALF), HALF)

    mine, other = half_cols(c), half_cols(1 - c)

    class Scatter:
        def __init__(self, part, rc, xs, rx, zs, rz):
            self.part, self.rc, self.xs, self.rx, self.zs, self.rz = part, rc, xs, rx, zs, rz
            self.ic = [net.slot() for _ in range(nz)]
            self.ix = [net.slot() for _ in range(nz)]
            self.iz = [net.slot() for _ in range(nz)]

        def block(self, o, value):
            rows = pair_rows(z_at(o))
            self.part[rows, :] = value
            net.send(self.ic[o], self.part.at[rows, other], self.rc.at[rows, :], core_peer)

        def over_x(self, o):
            rows = pair_rows(z_at(o))
            net.arrive(self.ic[o], self.rc.at[rows, :], core_peer)
            theirs = slab_rows(z_at(o), 1 - xl)
            self.xs[o] = self.part[theirs, mine] + self.rc[theirs, :]
            net.send(self.ix[o], self.xs.at[o], self.rx.at[o], x_peer)

        def over_z(self, o):
            net.arrive(self.ix[o], self.rx.at[o], x_peer)
            ours = slab_rows(z_at(o), xl)
            self.zs[o] = self.part[ours, mine] + self.rc[ours, :] + self.rx[o]
            if o:
                net.send(self.iz[o], self.zs.at[o], self.rz.at[o], z_peer(o))

        def total(self):
            value = self.zs[0]
            for o in near_first(nz):
                net.arrive(self.iz[o], self.rz.at[o], z_peer(o))
                value = value + self.rz[o]
            return value

    mixed = near_first(nz)[:2] + [o for o in far_first(nz) if o not in near_first(nz)[:2]]

    class Gather:
        def __init__(self, full):
            self.full = full
            self.ic = [net.slot() for _ in range(nz)]
            self.ix = [net.slot() for _ in range(nz)]
            self.iz = [net.slot() for _ in range(nz)]

        def over_z(self, value):
            rows = slab_rows(z, xl)
            self.full[rows, mine] = value
            chunk = self.full.at[rows, mine]
            net.send(self.ix[0], chunk, chunk, x_peer)
            for o in mixed:
                net.send(self.iz[o], chunk, chunk, z_peer(o))

        def over_x(self, o):
            chunk = self.full.at[slab_rows(z_at(nz - o), xl), mine]
            net.arrive(self.iz[o], chunk, z_peer(nz - o))
            net.send(self.ix[o], chunk, chunk, x_peer)

        def over_core(self, o):
            z_ = z_at(nz - o)
            net.arrive(self.ix[o], self.full.at[slab_rows(z_, 1 - xl), mine], x_peer)
            pair = self.full.at[pair_rows(z_), mine]
            net.send(self.ic[o], pair, pair, core_peer)

        def landed(self, o):
            net.arrive(self.ic[o], self.full.at[pair_rows(z_at(nz - o)), other], core_peer)

    class Sum:
        def __init__(self, buf, recv, zrecv):
            self.buf, self.recv, self.zrecv = buf, recv, zrecv
            self.ic, self.ix = net.slot(), net.slot()
            self.iz = [net.slot() for _ in range(nz)]

        def over_core(self):
            net.send(self.ic, self.buf.at[0], self.recv.at[0], core_peer)

        def over_x(self):
            net.arrive(self.ic, self.recv.at[0], core_peer)
            self.buf[1] = self.buf[0] + self.recv[0]
            net.send(self.ix, self.buf.at[1], self.recv.at[1], x_peer)

        def over_z(self):
            net.arrive(self.ix, self.recv.at[1], x_peer)
            self.buf[2] = self.buf[1] + self.recv[1]
            for o in far_first(nz):
                net.send(self.iz[o], self.buf.at[2], self.zrecv.at[o], z_peer(o))

        def total(self):
            value = self.buf[2]
            for o in near_first(nz):
                net.arrive(self.iz[o], self.zrecv.at[o], z_peer(o))
                value = value + self.zrecv[o]
            return value

    class SumA:
        def __init__(self, buf, recv, yrecv):
            self.buf, self.recv, self.yrecv = buf, recv, yrecv
            self.ix = net.slot()
            self.iy = [net.slot() for _ in range(ny)]

        def over_hi(self):
            net.send(self.ix, self.buf.at[0], self.recv, hi_peer)

        def over_y(self):
            net.arrive(self.ix, self.recv, hi_peer)
            self.buf[1] = self.buf[0] + self.recv[...]
            for o in far_first(ny):
                net.send(self.iy[o], self.buf.at[1], self.yrecv.at[o], y_peer(o))

        def total(self):
            value = self.buf[1]
            for o in near_first(ny):
                net.arrive(self.iy[o], self.yrecv.at[o], y_peer(o))
                value = value + self.yrecv[o]
            return value

    old_sum = Sum(abuf, arecv, azrecv)
    h_sum = SumA(hbuf, hrecv, hyrecv)
    image_sum = SumA(bbuf, brecv, byrecv)
    left_sum = Sum(fbuf, frecv, fzrecv)
    last_sum = Sum(cbuf, crecv, czrecv)

    first = Scatter(part, rc, xs, rx, zs, rz)
    gather = Gather(grad)

    def grad_block(i):
        act_loads[i].wait()
        return lax.dot_general(act[i], dy[...], TN, preferred_element_type=F32)

    def blocks_and_x(scatter, block_of, between=()):
        between = dict(between)
        for i in range(nz):
            scatter.block(z_order[i], block_of(i))
            if i in between:
                between[i]()
            if i >= 3:
                scatter.over_x(z_order[i - 3])
        for i in range(nz - 3, nz):
            if i >= 0:
                scatter.over_x(z_order[i])

    dy_load.wait()
    first_value = grad_block(0)
    pl.semaphore_wait(barrier, 5 + (nz - 1) + (ny - 1))
    blocks_and_x(first, lambda i: grad_block(i) if i else first_value)

    for copy in other_loads:
        copy.wait()
    row = lax.broadcasted_iota(jnp.int32, (8, 128), 0)
    p_row = jnp.broadcast_to(p_right[pl.ds(dp, 1), :], (8, 128))
    old_right = dot3(halves(p_row), halves(right_old[...]), NT)
    abuf[0] = jnp.where(row == 0, old_right[:, :HALF], old_right[:, HALF:])
    old_sum.over_core()
    for z_ in range(nz):
        prod[slab_rows(z_, 1 - xl), :] = jnp.zeros((SLAB, HALF), F32)
    for o in z_order[: nz // 2]:
        first.over_z(o)
    old_sum.over_x()
    for o in z_order[nz // 2 :]:
        first.over_z(o)
    old_sum.over_z()
    gown[...] = first.total()

    i_flip, i_flip_2 = net.slot(), net.slot()
    iy = [net.slot() for _ in range(ny)]
    ih = [net.slot() for _ in range(ny)]

    def panel_z(y_):
        return (z + y_ - b % ny + ny // 2 + nz) % nz

    def panel_slab(mp_, y_):
        return panel.at[slab_rows(panel_z(y_), jnp.where(mp_ == b // ny, xl, 1 - xl)), :]

    chunk = panel.at[slab_rows(z, xl), :]
    net.send(i_flip, gown, chunk, flip_to)
    net.send(i_flip_2, gown, chunk, flip_to_2)
    gather.over_z(gown[...])
    far = [o for o in far_first(ny) if min(o, ny - o) > 2]
    near = [o for o in far_first(ny) if min(o, ny - o) <= 2]
    net.arrive(i_flip, panel_slab(mp, pre), flip_from)
    for o in far:
        net.send(iy[o], panel_slab(mp, pre), panel_slab(mp, pre), y_peer(o))
    net.arrive(i_flip_2, panel_slab(1 - mp, pre), flip_from_2)
    own_pair = panel.at[pair_rows(panel_z(pre)), :]
    for o in near:
        net.send(iy[o], own_pair, own_pair, y_peer(o))
    for o in mixed:
        gather.over_x(o)
    core_order = [0] + mixed
    for o in core_order[: nz // 2 + 1]:
        gather.over_core(o)
    for o in reversed(far):
        slab = panel_slab(mp, y_at(ny - o))
        net.arrive(iy[o], slab, y_peer(ny - o))
        net.send(ih[o], slab, slab, hi_peer)
    for o in core_order[nz // 2 + 1 :]:
        gather.over_core(o)
    for o in core_order:
        gather.landed(o)

    il = [net.slot() for _ in range(ny)]
    ilx = net.slot()
    ilg = [net.slot() for _ in range(ny)]
    own32 = pl.ds(pl.multiple_of(dp * 32, 32), 32)
    grad_split = halves(grad[...])
    probe_a = jnp.concatenate([p_right[pl.ds(2 * a, 1), :], p_right[pl.ds(2 * a + 1, 1), :]], axis=1)
    rows40 = jnp.concatenate([grad[own32, :], jnp.broadcast_to(probe_a, (8, 2 * HALF))], axis=0)
    both = dot3(halves(rows40), grad_split, NT)
    for j in range(rows_l):
        hbuf[0, pl.ds(j, 1), :] = both[32:33, j * 128 : (j + 1) * 128]
    h_sum.over_hi()
    lpart[...] = both[0:32, :] * (1.0 / ff)
    old_lanes = pl.ds(pl.multiple_of((a // 2) * 128, 128), 128)
    old = left_old[...] * DECAY
    side = lax.broadcasted_iota(jnp.int32, (32, 128), 1) // SLAB
    lpart[:, old_lanes] += jnp.where(side == a % 2, jnp.concatenate([old, old], axis=1), 0.0)

    def l_lanes(y_):
        return pl.ds(pl.multiple_of(y_ * 128, 128), 128)

    for o in far_first(ny):
        net.send(il[o], lpart.at[:, l_lanes(y_at(o))], lr.at[o], y_peer(o))
    for o in near:
        net.arrive(iy[o], panel.at[pair_rows(panel_z(y_at(ny - o))), :], y_peer(ny - o))
    for o in reversed(far):
        net.arrive(ih[o], panel_slab(1 - mp, y_at(ny - o)), hi_peer)

    gram = dot3(halves(panel[...].T), grad_split, NN)
    rtile[...] = right_old[...].T * DECAY + gram * (1.0 / d_model)
    rt_split = halves(rtile[...])
    h_sum.over_y()

    second = Scatter(part2, rc2, xs2, rx2, zs2, rz2)

    def prod_block(i):
        return dot3(halves(panel[pair_rows(z_at(z_order[i])), :]), rt_split, NN)

    def right_images():
        h = h_sum.total()
        h_row = jnp.concatenate([h[j : j + 1, :] for j in range(rows_l)], axis=1)
        new = dot3(halves(jnp.broadcast_to(h_row, (8, d_model))), grad_split, NN)
        old_image = old_sum.total()
        f_old = jnp.concatenate([old_image[0:1, :], old_image[1:2, :]], axis=1)
        f_row = f_old * DECAY + new[0:1, :] * (1.0 / d_model)
        square = jnp.sum(f_row * f_row, axis=1, keepdims=True)
        image = dot3(halves(jnp.broadcast_to(f_row, (8, 2 * HALF))), rt_split, NT)
        bbuf[0] = jnp.where(row == 0, image, square)
        image_sum.over_hi()

    def left_rows():
        total = lpart[:, l_lanes(pre)]
        for o in near_first(ny):
            net.arrive(il[o], lr.at[o], y_peer(o))
            total = total + lr[o]
        lsum[...] = total
        net.send(ilx, lsum, lx, hi_peer)

    blocks_and_x(second, prod_block)
    left_rows()
    cut = [4, 5] if nz > 5 else [1, 1]
    for o in z_order[: cut[0]]:
        second.over_z(o)
    right_images()
    for o in z_order[cut[0] : cut[1]]:
        second.over_z(o)
    net.arrive(ilx, lx, hi_peer)
    lrow[:, l_lanes(pre)] = lsum[...] + lx[...]
    own_lanes = lrow.at[:, l_lanes(pre)]
    for o in far_first(ny):
        net.send(ilg[o], own_lanes, own_lanes, y_peer(o))
    for o in z_order[cut[1] :]:
        second.over_z(o)
    image_sum.over_y()

    for o in near_first(ny):
        net.arrive(ilg[o], lrow.at[:, l_lanes(y_at(ny - o))], y_peer(ny - o))

    def l_rows(xl_, c_):
        return lrows.at[pl.ds(pl.multiple_of((xl_ * 2 + c_) * 32, 32), 32), :]

    i_rows, i_rows_x, i_rows_xc = net.slot(), net.slot(), net.slot()
    net.send(i_rows_x, lrow, l_rows(xl, c), x_peer)
    net.send(i_rows, lrow, l_rows(xl, c), core_peer)
    l_rows(xl, c)[...] = lrow[...]
    f_left = jnp.zeros((32, 1), F32)
    for j in range(rows_l):
        f_left = f_left + jnp.sum(
            lrow[:, j * 128 : (j + 1) * 128] * p_left[pl.ds(j, 1), :], axis=1, keepdims=True
        )
    left_image = jnp.sum(lrow[...] * f_left, axis=0, keepdims=True)
    for j in range(rows_l):
        fbuf[0, pl.ds(j, 1), :] = left_image[:, j * 128 : (j + 1) * 128]
    left_square = jnp.sum(f_left * f_left, axis=0, keepdims=True)
    fbuf[0, pl.ds(rows_l, 8), :] = jnp.broadcast_to(left_square, (8, 128))
    left_sum.over_core()

    iz2 = [net.slot() for _ in range(nz)]
    i_prod, i_term_x, i_term_c = net.slot(), net.slot(), net.slot()
    prod[slab_rows(z, xl), :] = second.total()
    own_prod = prod.at[slab_rows(z, xl), :]
    for o in far_first(nz):
        net.send(iz2[o], own_prod, own_prod, z_peer(o))

    def rows_of(c_):
        return pl.ds(pl.multiple_of((z * 2 + xl) * SLAB + c_ * 32, 32), 32)

    net.send(i_prod, prod.at[rows_of(1 - c), :], wrow, core_peer)
    left_sum.over_x()

    whole = image_sum.total()
    norm_right = jnp.sqrt(whole[1:2, 0:1] + FLOOR)
    scaled = whole[0:1, :] / norm_right
    right_part = jnp.sum(scaled * scaled, axis=1, keepdims=True)
    cbuf[0] = jnp.broadcast_to(right_part, (8, 128))
    last_sum.over_core()

    left_grad = dot3(halves(lrow[...]), grad_split, NN)
    right_out[...] = rtile[...].T
    lanes = lrow[:, old_lanes]
    left_out[...] = jnp.where(a % 2 == 0, lanes[:, :SLAB], lanes[:, SLAB:])
    last_sum.over_x()
    left_sum.over_z()
    last_sum.over_z()
    net.arrive(i_rows_x, l_rows(1 - xl, c), x_peer)
    net.send(i_rows_xc, l_rows(1 - xl, c), l_rows(1 - xl, c), core_peer)
    net.arrive(i_rows, l_rows(xl, 1 - c), core_peer)
    net.arrive(i_rows_xc, l_rows(1 - xl, 1 - c), core_peer)

    term = jnp.zeros((128, HALF), F32)
    for o in [0] + [nz - o for o in far_first(nz)]:
        z_ = z_at(o)
        if o:
            net.arrive(iz2[nz - o], prod.at[slab_rows(z_, xl), :], z_peer(o))
        term = term + dot3(
            halves(lrows[:, l_lanes(z_)]), halves(prod[pair_rows(z_), :]), NN
        )
    terms[...] = term

    def term_rows(xl_):
        return pl.ds(pl.multiple_of(xl_ * SLAB, SLAB), SLAB)

    net.send(i_term_x, terms.at[term_rows(1 - xl), :], xterm, x_peer)
    top_right = jnp.sqrt(last_sum.total()[0:1, 0:1] + FLOOR)
    images = left_sum.total()
    norm_left = jnp.sqrt(images[rows_l : rows_l + 1, 0:1] + FLOOR)
    unit_image = images[0:rows_l, :] / norm_left
    top_left = jnp.sqrt(
        jnp.sum(jnp.sum(unit_image * unit_image, axis=1, keepdims=True), axis=0, keepdims=True)
        + FLOOR
    )
    scale = lax.rsqrt(jnp.sqrt(top_left * top_right)) * 0.0625
    rest = 5.0 * (5.0 * grad[own32, :] - left_grad / top_left)
    net.arrive(i_term_x, xterm, x_peer)
    sums[...] = terms[term_rows(xl), :] + xterm[...]

    def sum_rows(c_):
        return pl.ds(pl.multiple_of(c_ * 32, 32), 32)

    net.send(i_term_c, sums.at[sum_rows(1 - c), :], cterm, core_peer)
    update_out[...] = rest
    by_right = (sums[sum_rows(c), :] / top_left - 5.0 * prod[rows_of(c), :]) / top_right
    update_out[:, mine] = (update_out[:, mine] + by_right) * scale
    net.arrive(i_prod, wrow, core_peer)
    net.arrive(i_term_c, cterm, core_peer)
    by_right = (cterm[...] / top_left - 5.0 * wrow[...]) / top_right
    update_out[:, other] = (update_out[:, other] + by_right) * scale

    net.finish()


def store(left, right, update, left_out, right_out, update_out, sem):
    pairs = ((left, left_out), (right, right_out), (update, update_out))
    copies = [pltpu.make_async_copy(src, dst, sem.at[i]) for i, (src, dst) in enumerate(pairs)]
    for copy in copies:
        copy.start()
    for copy in copies:
        copy.wait()


def step(nz, ny, ff, activations, grad_output, left_old, right_old, probe_left, probe_right):
    d_model = activations.shape[1]
    block = grad_output.shape[1]
    rows_l = d_model // 128
    vmem = pltpu.VMEM

    def scatter_bufs(columns):
        return [
            vmem((d_model, block), F32),
            vmem((d_model, HALF), F32),
            vmem((nz, SLAB, HALF), F32),
            vmem((nz, SLAB, HALF), F32),
            vmem((nz, SLAB, HALF), F32),
            vmem((nz, SLAB, HALF), F32),
            vmem((d_model, columns), F32),
        ]

    scratch = [
        vmem((nz, activations.shape[0], 128), BF16),
        vmem(grad_output.shape, BF16),
        vmem((left_old.shape[1], left_old.shape[0]), F32),
        vmem(right_old.shape, F32),
        vmem((probe_left.shape[0] // 128, 128), F32),
        vmem((probe_right.shape[0] // 128, 128), F32),
        *scatter_bufs(block),
        *scatter_bufs(HALF),
        vmem((SLAB, HALF), F32),
        vmem((d_model, HALF), F32),
        vmem((HALF, block), F32),
        vmem((32, d_model), F32),
        vmem((ny, 32, 128), F32),
        vmem((32, 128), F32),
        vmem((32, 128), F32),
        vmem((32, d_model), F32),
        vmem((128, d_model), F32),
        vmem((128, HALF), F32),
        vmem((SLAB, HALF), F32),
        vmem((SLAB, HALF), F32),
        vmem((32, HALF), F32),
        vmem((32, HALF), F32),
        vmem((3, 8, 128), F32),
        vmem((2, 8, 128), F32),
        vmem((nz, 8, 128), F32),
        vmem((2, rows_l, 128), F32),
        vmem((rows_l, 128), F32),
        vmem((ny, rows_l, 128), F32),
        vmem((3, rows_l + 8, 128), F32),
        vmem((2, rows_l + 8, 128), F32),
        vmem((nz, rows_l + 8, 128), F32),
        vmem((2, 8, 128), F32),
        vmem((8, 128), F32),
        vmem((ny, 8, 128), F32),
        vmem((3, 8, 128), F32),
        vmem((2, 8, 128), F32),
        vmem((nz, 8, 128), F32),
        pltpu.SemaphoreType.DMA((COPIES,)),
        pltpu.SemaphoreType.DMA((COPIES,)),
        pltpu.SemaphoreType.DMA((nz + 5,)),
    ]
    spec = pl.BlockSpec(memory_space=pltpu.VMEM)
    left, right, update = pl.pallas_call(
        functools.partial(kernel, nz, ny, ff),
        out_shape=(
            jax.ShapeDtypeStruct((left_old.shape[1], left_old.shape[0]), F32),
            jax.ShapeDtypeStruct(right_old.shape, F32),
            jax.ShapeDtypeStruct((d_model // (4 * nz), block), F32),
        ),
        in_specs=[pl.BlockSpec(memory_space=pltpu.HBM)] * 6,
        out_specs=(spec,) * 3,
        scratch_shapes=scratch,
        compiler_params=pltpu.CompilerParams(
            collective_id=0, has_side_effects=True, vmem_limit_bytes=58 * 1024 * 1024
        ),
        name="shampoo",
    )(
        activations,
        grad_output,
        left_old.T,
        right_old,
        probe_left.reshape(-1, 128),
        probe_right.reshape(-1, 128),
    )
    left, right, update = pl.pallas_call(
        store,
        out_shape=tuple(jax.ShapeDtypeStruct(r.shape, F32) for r in (left, right, update)),
        in_specs=[spec] * 3,
        out_specs=(pl.BlockSpec(memory_space=pltpu.HBM),) * 3,
        scratch_shapes=[pltpu.SemaphoreType.DMA((3,))],
        name="store",
    )(left, right, update)
    return left.T, right, update


def solution(mesh):
    nz = mesh.shape["dp"] // 4
    ny = mesh.shape["pre"]
    in_specs = (
        P("dp", None),
        P("dp", ("mp", "pre")),
        P(("mp", "pre"), "dp"),
        P(("mp", "pre"), "dp"),
        P(),
        P(),
    )
    out_specs = (P(("mp", "pre"), "dp"), P(("mp", "pre"), "dp"), P("dp", ("mp", "pre")))
    ff = 2 * ny * 2 * HALF
    return jax.shard_map(
        functools.partial(step, nz, ny, ff),
        mesh=mesh,
        in_specs=in_specs,
        out_specs=out_specs,
        check_vma=False,
    )
```

```python
import functools

import jax
import jax.numpy as jnp
from jax import lax
from jax.experimental import pallas as pl
from jax.experimental.pallas import tpu as pltpu
from jax.sharding import PartitionSpec as P

MESH = pl.DeviceIdType.MESH
F32 = jnp.float32
BF16 = jnp.bfloat16

DECAY = 0.9
FLOOR = 1e-06
SLAB = 64
HALF = 128
COPIES = 216

NN = (((1,), (0,)), ((), ()))
NT = (((1,), (1,)), ((), ()))
TN = (((0,), (0,)), ((), ()))


def far_first(n):
    return sorted(range(1, n), key=lambda o: -min(o, n - o))


def near_first(n):
    return sorted(range(1, n), key=lambda o: min(o, n - o))


def halves(v):
    high = v.astype(BF16)
    return high, (v - high.astype(F32)).astype(BF16)


def dot3(a, b, dims):
    (ah, al), (bh, bl) = a, b
    dot = functools.partial(lax.dot_general, dimension_numbers=dims, preferred_element_type=F32)
    return dot(ah, bh) + (dot(ah, bl) + dot(al, bh))


class Net:
    def __init__(self, send_sem, recv_sem):
        self.send_sem, self.recv_sem, self.used, self.sent = send_sem, recv_sem, 0, []

    def slot(self):
        self.used += 1
        assert self.used <= COPIES
        return self.used - 1

    def copy(self, i, src, dst, device):
        return pltpu.make_async_remote_copy(
            src_ref=src,
            dst_ref=dst,
            send_sem=self.send_sem.at[i],
            recv_sem=self.recv_sem.at[i],
            device_id=device,
            device_id_type=MESH,
        )

    def send(self, i, src, dst, device):
        copy = self.copy(i, src, dst, device)
        copy.start()
        self.sent.append(copy)

    def arrive(self, i, dst, device):
        self.copy(i, dst, dst, device).wait_recv()

    def finish(self):
        for copy in self.sent:
            copy.wait_send()


def kernel(
    nz,
    ny,
    ff,
    act_hbm,
    dy_hbm,
    left_hbm,
    right_hbm,
    p_left_hbm,
    p_right_hbm,
    left_out,
    right_out,
    update_out,
    act,
    dy,
    left_old,
    right_old,
    p_left,
    p_right,
    part,
    rc,
    xs,
    rx,
    zs,
    rz,
    grad,
    part2,
    rc2,
    xs2,
    rx2,
    zs2,
    rz2,
    prod,
    gown,
    panel,
    rtile,
    lpart,
    lr,
    lsum,
    lx,
    lrow,
    lrows,
    terms,
    tcore,
    tx,
    tcross,
    wrow,
    abuf,
    arecv,
    azrecv,
    hbuf,
    hrecv,
    hyrecv,
    fbuf,
    frecv,
    fzrecv,
    bbuf,
    brecv,
    byrecv,
    cbuf,
    crecv,
    czrecv,
    send_sem,
    recv_sem,
    load_sem,
):
    d_model = nz * 2 * SLAB
    rows_l = d_model // 128
    dp, mp, pre = lax.axis_index("dp"), lax.axis_index("mp"), lax.axis_index("pre")
    z, xl, c = dp // 4, (dp // 2) % 2, dp % 2
    a = mp * ny + pre
    b = z * 2 + xl
    core_peer = (dp + 1 - 2 * c, mp, pre)
    x_peer = (dp + 2 - 4 * xl, mp, pre)
    hi_peer = (dp, 1 - mp, pre)
    cross_peer = (dp + 3 - 4 * xl - 2 * c, mp, pre)
    quad = (core_peer, x_peer, cross_peer)

    turn = (z - a // 2 + ny // 2 + nz) % nz
    goal_hi = jnp.where(xl == a % 2, mp, 1 - mp)
    flip_to = (a * 2 + c, goal_hi, (pre + turn) % ny)
    came = (z + pre - b % ny + ny // 2 + nz) % nz
    came_lo = jnp.where(mp == b // ny, xl, 1 - xl)
    flip_from = (came * 4 + came_lo * 2 + c, b // ny, b % ny)
    flip_to_2 = (a * 2 + c, 1 - goal_hi, (pre + turn) % ny)
    flip_from_2 = (came * 4 + (1 - came_lo) * 2 + c, b // ny, b % ny)

    def z_at(o):
        return (z + o) % nz

    def z_peer(o):
        return (z_at(o) * 4 + xl * 2 + c, mp, pre)

    def y_at(o):
        return (pre + o) % ny

    def y_peer(o):
        return (dp, mp, y_at(o))

    net = Net(send_sem, recv_sem)

    barrier = pltpu.get_barrier_semaphore()

    def greet(device):
        pl.semaphore_signal(barrier, inc=1, device_id=device, device_id_type=MESH)

    loads = []

    def load(src, dst):
        copy = pltpu.make_async_copy(src, dst, load_sem.at[len(loads)])
        copy.start()
        loads.append(copy)
        return copy

    def act_cols(o):
        return pl.ds(pl.multiple_of(z_at(o) * 128, 128), 128)

    z_order = far_first(nz) + [0]
    dy_load = load(dy_hbm, dy)
    act_loads = [load(act_hbm.at[:, act_cols(o)], act.at[i]) for i, o in enumerate(z_order)]
    other_loads = [
        load(left_hbm, left_old),
        load(right_hbm, right_old),
        load(p_left_hbm, p_left),
        load(p_right_hbm, p_right),
    ]

    greet(core_peer)
    greet(x_peer)
    greet(hi_peer)
    greet(cross_peer)
    for o in range(1, nz):
        greet(z_peer(o))
    for o in range(1, ny):
        greet(y_peer(o))

    greet(flip_from)
    greet(flip_from_2)

    def slab_rows(z_, xl_):
        return pl.ds(pl.multiple_of((z_ * 2 + xl_) * SLAB, SLAB), SLAB)

    def pair_rows(z_):
        return pl.ds(pl.multiple_of(z_ * 2 * SLAB, 2 * SLAB), 2 * SLAB)

    def half_cols(c_):
        return pl.ds(pl.multiple_of(c_ * HALF, HALF), HALF)

    mine, other = half_cols(c), half_cols(1 - c)

    class Scatter:
        def __init__(self, part, rc, xs, rx, zs, rz):
            self.part, self.rc, self.xs, self.rx, self.zs, self.rz = part, rc, xs, rx, zs, rz
            self.ic = [net.slot() for _ in range(nz)]
            self.ix = [net.slot() for _ in range(nz)]
            self.iz = [net.slot() for _ in range(nz)]

        def block(self, o, value):
            rows = pair_rows(z_at(o))
            self.part[rows, :] = value
            net.send(self.ic[o], self.part.at[rows, other], self.rc.at[rows, :], core_peer)

        def over_x(self, o):
            rows = pair_rows(z_at(o))
            net.arrive(self.ic[o], self.rc.at[rows, :], core_peer)
            theirs = slab_rows(z_at(o), 1 - xl)
            self.xs[o] = self.part[theirs, mine] + self.rc[theirs, :]
            net.send(self.ix[o], self.xs.at[o], self.rx.at[o], x_peer)

        def over_z(self, o):
            net.arrive(self.ix[o], self.rx.at[o], x_peer)
            ours = slab_rows(z_at(o), xl)
            self.zs[o] = self.part[ours, mine] + self.rc[ours, :] + self.rx[o]
            if o:
                net.send(self.iz[o], self.zs.at[o], self.rz.at[o], z_peer(o))

        def total(self):
            value = self.zs[0]
            for o in near_first(nz):
                net.arrive(self.iz[o], self.rz.at[o], z_peer(o))
                value = value + self.rz[o]
            return value

    mixed = near_first(nz)[:2] + [o for o in far_first(nz) if o not in near_first(nz)[:2]]

    class Gather:
        def __init__(self, full):
            self.full = full
            self.ic = [net.slot() for _ in range(nz)]
            self.ix = [net.slot() for _ in range(nz)]
            self.iz = [net.slot() for _ in range(nz)]

        def over_z(self, value):
            rows = slab_rows(z, xl)
            self.full[rows, mine] = value
            chunk = self.full.at[rows, mine]
            net.send(self.ix[0], chunk, chunk, x_peer)
            for o in mixed:
                net.send(self.iz[o], chunk, chunk, z_peer(o))

        def over_x(self, o):
            chunk = self.full.at[slab_rows(z_at(nz - o), xl), mine]
            net.arrive(self.iz[o], chunk, z_peer(nz - o))
            net.send(self.ix[o], chunk, chunk, x_peer)

        def over_core(self, o):
            z_ = z_at(nz - o)
            net.arrive(self.ix[o], self.full.at[slab_rows(z_, 1 - xl), mine], x_peer)
            pair = self.full.at[pair_rows(z_), mine]
            net.send(self.ic[o], pair, pair, core_peer)

        def landed(self, o):
            net.arrive(self.ic[o], self.full.at[pair_rows(z_at(nz - o)), other], core_peer)

    class Sum:
        def __init__(self, buf, recv, zrecv):
            self.buf, self.recv, self.zrecv = buf, recv, zrecv
            self.iq = [net.slot() for _ in quad]
            self.iz = [net.slot() for _ in range(nz)]

        def over_quad(self):
            for i, peer in zip(self.iq, quad):
                net.send(i, self.buf.at[0], self.recv.at[i - self.iq[0]], peer)

        def over_z(self):
            value = self.buf[0]
            for i, peer in zip(self.iq, quad):
                net.arrive(i, self.recv.at[i - self.iq[0]], peer)
                value = value + self.recv[i - self.iq[0]]
            self.buf[1] = value
            for o in far_first(nz):
                net.send(self.iz[o], self.buf.at[1], self.zrecv.at[o], z_peer(o))

        def total(self):
            value = self.buf[1]
            for o in near_first(nz):
                net.arrive(self.iz[o], self.zrecv.at[o], z_peer(o))
                value = value + self.zrecv[o]
            return value

    class SumA:
        def __init__(self, buf, recv, yrecv):
            self.buf, self.recv, self.yrecv = buf, recv, yrecv
            self.ix = net.slot()
            self.iy = [net.slot() for _ in range(ny)]

        def over_hi(self):
            net.send(self.ix, self.buf.at[0], self.recv, hi_peer)

        def over_y(self):
            net.arrive(self.ix, self.recv, hi_peer)
            self.buf[1] = self.buf[0] + self.recv[...]
            for o in far_first(ny):
                net.send(self.iy[o], self.buf.at[1], self.yrecv.at[o], y_peer(o))

        def total(self):
            value = self.buf[1]
            for o in near_first(ny):
                net.arrive(self.iy[o], self.yrecv.at[o], y_peer(o))
                value = value + self.yrecv[o]
            return value

    old_sum = Sum(abuf, arecv, azrecv)
    h_sum = SumA(hbuf, hrecv, hyrecv)
    image_sum = SumA(bbuf, brecv, byrecv)
    left_sum = Sum(fbuf, frecv, fzrecv)
    last_sum = Sum(cbuf, crecv, czrecv)

    first = Scatter(part, rc, xs, rx, zs, rz)
    gather = Gather(grad)

    def grad_block(i):
        act_loads[i].wait()
        return lax.dot_general(act[i], dy[...], TN, preferred_element_type=F32)

    def blocks_and_x(scatter, block_of, between=()):
        between = dict(between)
        for i in range(nz):
            scatter.block(z_order[i], block_of(i))
            if i in between:
                between[i]()
            if i >= 3:
                scatter.over_x(z_order[i - 3])
        for i in range(nz - 3, nz):
            if i >= 0:
                scatter.over_x(z_order[i])

    dy_load.wait()
    first_value = grad_block(0)
    pl.semaphore_wait(barrier, 6 + (nz - 1) + (ny - 1))
    blocks_and_x(first, lambda i: grad_block(i) if i else first_value)

    for copy in other_loads:
        copy.wait()
    row = lax.broadcasted_iota(jnp.int32, (8, 128), 0)
    p_row = jnp.broadcast_to(p_right[pl.ds(dp, 1), :], (8, 128))
    old_right = dot3(halves(p_row), halves(right_old[...]), NT)
    abuf[0] = jnp.where(row == 0, old_right[:, :HALF], old_right[:, HALF:])
    old_sum.over_quad()
    for z_ in range(nz):
        prod[slab_rows(z_, 1 - xl), :] = jnp.zeros((SLAB, HALF), F32)
    for o in z_order[: nz // 2]:
        first.over_z(o)
    for o in z_order[nz // 2 :]:
        first.over_z(o)
    old_sum.over_z()
    gown[...] = first.total()

    i_flip, i_flip_2 = net.slot(), net.slot()
    iy = [net.slot() for _ in range(ny)]
    ih = [net.slot() for _ in range(ny)]

    def panel_z(y_):
        return (z + y_ - b % ny + ny // 2 + nz) % nz

    def panel_slab(mp_, y_):
        return panel.at[slab_rows(panel_z(y_), jnp.where(mp_ == b // ny, xl, 1 - xl)), :]

    chunk = panel.at[slab_rows(z, xl), :]
    net.send(i_flip, gown, chunk, flip_to)
    net.send(i_flip_2, gown, chunk, flip_to_2)
    gather.over_z(gown[...])
    far = [o for o in far_first(ny) if min(o, ny - o) > 2]
    near = [o for o in far_first(ny) if min(o, ny - o) <= 2]
    net.arrive(i_flip, panel_slab(mp, pre), flip_from)
    for o in far:
        net.send(iy[o], panel_slab(mp, pre), panel_slab(mp, pre), y_peer(o))
    net.arrive(i_flip_2, panel_slab(1 - mp, pre), flip_from_2)
    own_pair = panel.at[pair_rows(panel_z(pre)), :]
    for o in near:
        net.send(iy[o], own_pair, own_pair, y_peer(o))
    for o in mixed:
        gather.over_x(o)
    core_order = [0] + mixed
    for o in core_order[: nz // 2 + 1]:
        gather.over_core(o)
    for o in reversed(far):
        slab = panel_slab(mp, y_at(ny - o))
        net.arrive(iy[o], slab, y_peer(ny - o))
        net.send(ih[o], slab, slab, hi_peer)
    for o in core_order[nz // 2 + 1 :]:
        gather.over_core(o)
    for o in core_order:
        gather.landed(o)

    il = [net.slot() for _ in range(ny)]
    ilx = net.slot()
    ilg = [net.slot() for _ in range(ny)]
    own32 = pl.ds(pl.multiple_of(dp * 32, 32), 32)
    grad_split = halves(grad[...])
    probe_a = jnp.concatenate([p_right[pl.ds(2 * a, 1), :], p_right[pl.ds(2 * a + 1, 1), :]], axis=1)
    rows40 = jnp.concatenate([grad[own32, :], jnp.broadcast_to(probe_a, (8, 2 * HALF))], axis=0)
    both = dot3(halves(rows40), grad_split, NT)
    for j in range(rows_l):
        hbuf[0, pl.ds(j, 1), :] = both[32:33, j * 128 : (j + 1) * 128]
    h_sum.over_hi()
    lpart[...] = both[0:32, :] * (1.0 / ff)
    old_lanes = pl.ds(pl.multiple_of((a // 2) * 128, 128), 128)
    old = left_old[...] * DECAY
    side = lax.broadcasted_iota(jnp.int32, (32, 128), 1) // SLAB
    lpart[:, old_lanes] += jnp.where(side == a % 2, jnp.concatenate([old, old], axis=1), 0.0)

    def l_lanes(y_):
        return pl.ds(pl.multiple_of(y_ * 128, 128), 128)

    for o in far_first(ny):
        net.send(il[o], lpart.at[:, l_lanes(y_at(o))], lr.at[o], y_peer(o))
    for o in near:
        net.arrive(iy[o], panel.at[pair_rows(panel_z(y_at(ny - o))), :], y_peer(ny - o))
    for o in reversed(far):
        net.arrive(ih[o], panel_slab(1 - mp, y_at(ny - o)), hi_peer)

    gram = dot3(halves(panel[...].T), grad_split, NN)
    rtile[...] = right_old[...].T * DECAY + gram * (1.0 / d_model)
    rt_split = halves(rtile[...])
    h_sum.over_y()

    second = Scatter(part2, rc2, xs2, rx2, zs2, rz2)

    def prod_block(i):
        return dot3(halves(panel[pair_rows(z_at(z_order[i])), :]), rt_split, NN)

    def right_images():
        h = h_sum.total()
        h_row = jnp.concatenate([h[j : j + 1, :] for j in range(rows_l)], axis=1)
        new = dot3(halves(jnp.broadcast_to(h_row, (8, d_model))), grad_split, NN)
        old_image = old_sum.total()
        f_old = jnp.concatenate([old_image[0:1, :], old_image[1:2, :]], axis=1)
        f_row = f_old * DECAY + new[0:1, :] * (1.0 / d_model)
        square = jnp.sum(f_row * f_row, axis=1, keepdims=True)
        image = dot3(halves(jnp.broadcast_to(f_row, (8, 2 * HALF))), rt_split, NT)
        bbuf[0] = jnp.where(row == 0, image, square)
        image_sum.over_hi()

    def left_rows():
        total = lpart[:, l_lanes(pre)]
        for o in near_first(ny):
            net.arrive(il[o], lr.at[o], y_peer(o))
            total = total + lr[o]
        lsum[...] = total
        net.send(ilx, lsum, lx, hi_peer)

    blocks_and_x(second, prod_block)
    left_rows()
    cut = [2, 4, 7] if nz > 6 else [1, 1, 1]
    for o in z_order[: cut[0]]:
        second.over_z(o)
    right_images()
    for o in z_order[cut[0] : cut[1]]:
        second.over_z(o)
    net.arrive(ilx, lx, hi_peer)
    lrow[:, l_lanes(pre)] = lsum[...] + lx[...]
    own_lanes = lrow.at[:, l_lanes(pre)]
    for o in far_first(ny):
        net.send(ilg[o], own_lanes, own_lanes, y_peer(o))
    for o in z_order[cut[1] : cut[2]]:
        second.over_z(o)
    image_sum.over_y()
    for o in z_order[cut[2] :]:
        second.over_z(o)

    for o in near_first(ny):
        net.arrive(ilg[o], lrow.at[:, l_lanes(y_at(ny - o))], y_peer(ny - o))

    def l_rows(xl_, c_):
        return lrows.at[pl.ds(pl.multiple_of((xl_ * 2 + c_) * 32, 32), 32), :]

    i_rows, i_rows_x, i_rows_xc = net.slot(), net.slot(), net.slot()
    net.send(i_rows_x, lrow, l_rows(xl, c), x_peer)
    net.send(i_rows, lrow, l_rows(xl, c), core_peer)
    l_rows(xl, c)[...] = lrow[...]
    f_left = jnp.zeros((32, 1), F32)
    for j in range(rows_l):
        f_left = f_left + jnp.sum(
            lrow[:, j * 128 : (j + 1) * 128] * p_left[pl.ds(j, 1), :], axis=1, keepdims=True
        )
    left_image = jnp.sum(lrow[...] * f_left, axis=0, keepdims=True)
    for j in range(rows_l):
        fbuf[0, pl.ds(j, 1), :] = left_image[:, j * 128 : (j + 1) * 128]
    left_square = jnp.sum(f_left * f_left, axis=0, keepdims=True)
    fbuf[0, pl.ds(rows_l, 8), :] = jnp.broadcast_to(left_square, (8, 128))
    left_sum.over_quad()

    whole = image_sum.total()
    norm_right = jnp.sqrt(whole[1:2, 0:1] + FLOOR)
    scaled = whole[0:1, :] / norm_right
    right_part = jnp.sum(scaled * scaled, axis=1, keepdims=True)
    cbuf[0] = jnp.broadcast_to(right_part, (8, 128))
    last_sum.over_quad()

    iz2 = [net.slot() for _ in range(nz)]
    i_prod = net.slot()
    i_term = [net.slot() for _ in quad]
    prod[slab_rows(z, xl), :] = second.total()
    own_prod = prod.at[slab_rows(z, xl), :]
    for o in far_first(nz):
        net.send(iz2[o], own_prod, own_prod, z_peer(o))

    def rows_of(c_):
        return pl.ds(pl.multiple_of((z * 2 + xl) * SLAB + c_ * 32, 32), 32)

    net.send(i_prod, prod.at[rows_of(1 - c), :], wrow, core_peer)

    left_grad = dot3(halves(lrow[...]), grad_split, NN)
    right_out[...] = rtile[...].T
    lanes = lrow[:, old_lanes]
    left_out[...] = jnp.where(a % 2 == 0, lanes[:, :SLAB], lanes[:, SLAB:])
    left_sum.over_z()
    last_sum.over_z()
    net.arrive(i_rows_x, l_rows(1 - xl, c), x_peer)
    net.send(i_rows_xc, l_rows(1 - xl, c), l_rows(1 - xl, c), core_peer)
    net.arrive(i_rows, l_rows(xl, 1 - c), core_peer)
    net.arrive(i_rows_xc, l_rows(1 - xl, 1 - c), core_peer)

    term = jnp.zeros((128, HALF), F32)
    for o in [0] + [nz - o for o in far_first(nz)]:
        z_ = z_at(o)
        if o:
            net.arrive(iz2[nz - o], prod.at[slab_rows(z_, xl), :], z_peer(o))
        term = term + dot3(
            halves(lrows[:, l_lanes(z_)]), halves(prod[pair_rows(z_), :]), NN
        )
    terms[...] = term

    def term_rows(xl_, c_):
        return pl.ds(pl.multiple_of((xl_ * 2 + c_) * 32, 32), 32)

    net.send(i_term[1], terms.at[term_rows(1 - xl, c), :], tx, x_peer)
    net.send(i_term[2], terms.at[term_rows(1 - xl, 1 - c), :], tcross, cross_peer)
    net.send(i_term[0], terms.at[term_rows(xl, 1 - c), :], tcore, core_peer)
    top_right = jnp.sqrt(last_sum.total()[0:1, 0:1] + FLOOR)
    images = left_sum.total()
    norm_left = jnp.sqrt(images[rows_l : rows_l + 1, 0:1] + FLOOR)
    unit_image = images[0:rows_l, :] / norm_left
    top_left = jnp.sqrt(
        jnp.sum(jnp.sum(unit_image * unit_image, axis=1, keepdims=True), axis=0, keepdims=True)
        + FLOOR
    )
    scale = lax.rsqrt(jnp.sqrt(top_left * top_right)) * 0.0625
    rest = 5.0 * (5.0 * grad[own32, :] - left_grad / top_left)
    update_out[...] = rest
    net.arrive(i_prod, wrow, core_peer)
    net.arrive(i_term[0], tcore, core_peer)
    net.arrive(i_term[1], tx, x_peer)
    by_right = ((terms[term_rows(xl, c), :] + tx[...]) / top_left - 5.0 * prod[rows_of(c), :]) / top_right
    update_out[:, mine] = (update_out[:, mine] + by_right) * scale
    net.arrive(i_term[2], tcross, cross_peer)
    by_right = ((tcore[...] + tcross[...]) / top_left - 5.0 * wrow[...]) / top_right
    update_out[:, other] = (update_out[:, other] + by_right) * scale

    net.finish()


def store(left, right, update, left_out, right_out, update_out, sem):
    pairs = ((left, left_out), (right, right_out), (update, update_out))
    copies = [pltpu.make_async_copy(src, dst, sem.at[i]) for i, (src, dst) in enumerate(pairs)]
    for copy in copies:
        copy.start()
    for copy in copies:
        copy.wait()


def step(nz, ny, ff, activations, grad_output, left_old, right_old, probe_left, probe_right):
    d_model = activations.shape[1]
    block = grad_output.shape[1]
    rows_l = d_model // 128
    vmem = pltpu.VMEM

    def scatter_bufs(columns):
        return [
            vmem((d_model, block), F32),
            vmem((d_model, HALF), F32),
            vmem((nz, SLAB, HALF), F32),
            vmem((nz, SLAB, HALF), F32),
            vmem((nz, SLAB, HALF), F32),
            vmem((nz, SLAB, HALF), F32),
            vmem((d_model, columns), F32),
        ]

    scratch = [
        vmem((nz, activations.shape[0], 128), BF16),
        vmem(grad_output.shape, BF16),
        vmem((left_old.shape[1], left_old.shape[0]), F32),
        vmem(right_old.shape, F32),
        vmem((probe_left.shape[0] // 128, 128), F32),
        vmem((probe_right.shape[0] // 128, 128), F32),
        *scatter_bufs(block),
        *scatter_bufs(HALF),
        vmem((SLAB, HALF), F32),
        vmem((d_model, HALF), F32),
        vmem((HALF, block), F32),
        vmem((32, d_model), F32),
        vmem((ny, 32, 128), F32),
        vmem((32, 128), F32),
        vmem((32, 128), F32),
        vmem((32, d_model), F32),
        vmem((128, d_model), F32),
        vmem((128, HALF), F32),
        vmem((32, HALF), F32),
        vmem((32, HALF), F32),
        vmem((32, HALF), F32),
        vmem((32, HALF), F32),
        vmem((2, 8, 128), F32),
        vmem((3, 8, 128), F32),
        vmem((nz, 8, 128), F32),
        vmem((2, rows_l, 128), F32),
        vmem((rows_l, 128), F32),
        vmem((ny, rows_l, 128), F32),
        vmem((2, rows_l + 8, 128), F32),
        vmem((3, rows_l + 8, 128), F32),
        vmem((nz, rows_l + 8, 128), F32),
        vmem((2, 8, 128), F32),
        vmem((8, 128), F32),
        vmem((ny, 8, 128), F32),
        vmem((2, 8, 128), F32),
        vmem((3, 8, 128), F32),
        vmem((nz, 8, 128), F32),
        pltpu.SemaphoreType.DMA((COPIES,)),
        pltpu.SemaphoreType.DMA((COPIES,)),
        pltpu.SemaphoreType.DMA((nz + 5,)),
    ]
    spec = pl.BlockSpec(memory_space=pltpu.VMEM)
    left, right, update = pl.pallas_call(
        functools.partial(kernel, nz, ny, ff),
        out_shape=(
            jax.ShapeDtypeStruct((left_old.shape[1], left_old.shape[0]), F32),
            jax.ShapeDtypeStruct(right_old.shape, F32),
            jax.ShapeDtypeStruct((d_model // (4 * nz), block), F32),
        ),
        in_specs=[pl.BlockSpec(memory_space=pltpu.HBM)] * 6,
        out_specs=(spec,) * 3,
        scratch_shapes=scratch,
        compiler_params=pltpu.CompilerParams(
            collective_id=0, has_side_effects=True, vmem_limit_bytes=58 * 1024 * 1024
        ),
        name="shampoo",
    )(
        activations,
        grad_output,
        left_old.T,
        right_old,
        probe_left.reshape(-1, 128),
        probe_right.reshape(-1, 128),
    )
    left, right, update = pl.pallas_call(
        store,
        out_shape=tuple(jax.ShapeDtypeStruct(r.shape, F32) for r in (left, right, update)),
        in_specs=[spec] * 3,
        out_specs=(pl.BlockSpec(memory_space=pltpu.HBM),) * 3,
        scratch_shapes=[pltpu.SemaphoreType.DMA((3,))],
        name="store",
    )(left, right, update)
    return left.T, right, update


def solution(mesh):
    nz = mesh.shape["dp"] // 4
    ny = mesh.shape["pre"]
    in_specs = (
        P("dp", None),
        P("dp", ("mp", "pre")),
        P(("mp", "pre"), "dp"),
        P(("mp", "pre"), "dp"),
        P(),
        P(),
    )
    out_specs = (P(("mp", "pre"), "dp"), P(("mp", "pre"), "dp"), P("dp", ("mp", "pre")))
    ff = 2 * ny * 2 * HALF
    return jax.shard_map(
        functools.partial(step, nz, ny, ff),
        mesh=mesh,
        in_specs=in_specs,
        out_specs=out_specs,
        check_vma=False,
    )
```

```python
import functools

import jax
import jax.numpy as jnp
from jax import lax
from jax.experimental import pallas as pl
from jax.experimental.pallas import tpu as pltpu
from jax.sharding import PartitionSpec as P

MESH = pl.DeviceIdType.MESH
F32 = jnp.float32
BF16 = jnp.bfloat16

DECAY = 0.9
FLOOR = 1e-06
SLAB = 64
HALF = 128
COPIES = 216

NN = (((1,), (0,)), ((), ()))
NT = (((1,), (1,)), ((), ()))
TN = (((0,), (0,)), ((), ()))


def far_first(n):
    return sorted(range(1, n), key=lambda o: -min(o, n - o))


def near_first(n):
    return sorted(range(1, n), key=lambda o: min(o, n - o))


def halves(v):
    high = v.astype(BF16)
    return high, (v - high.astype(F32)).astype(BF16)


def dot3(a, b, dims):
    (ah, al), (bh, bl) = a, b
    dot = functools.partial(lax.dot_general, dimension_numbers=dims, preferred_element_type=F32)
    return dot(ah, bh) + (dot(ah, bl) + dot(al, bh))


class Net:
    def __init__(self, send_sem, recv_sem):
        self.send_sem, self.recv_sem, self.used, self.sent = send_sem, recv_sem, 0, []

    def slot(self):
        self.used += 1
        assert self.used <= COPIES
        return self.used - 1

    def copy(self, i, src, dst, device):
        return pltpu.make_async_remote_copy(
            src_ref=src,
            dst_ref=dst,
            send_sem=self.send_sem.at[i],
            recv_sem=self.recv_sem.at[i],
            device_id=device,
            device_id_type=MESH,
        )

    def send(self, i, src, dst, device):
        copy = self.copy(i, src, dst, device)
        copy.start()
        self.sent.append(copy)

    def arrive(self, i, dst, device):
        self.copy(i, dst, dst, device).wait_recv()

    def finish(self):
        for copy in self.sent:
            copy.wait_send()


def kernel(
    nz,
    ny,
    ff,
    act_hbm,
    dy_hbm,
    left_hbm,
    right_hbm,
    p_left_hbm,
    p_right_hbm,
    left_out,
    right_out,
    update_out,
    act,
    dy,
    left_old,
    right_old,
    p_left,
    p_right,
    part,
    rc,
    xs,
    rx,
    zs,
    rz,
    grad,
    part2,
    rc2,
    xs2,
    rx2,
    zs2,
    rz2,
    prod,
    gown,
    panel,
    rtile,
    lpart,
    lr,
    lsum,
    lx,
    lrow,
    lrows,
    terms,
    tcore,
    tx,
    tcross,
    wrow,
    abuf,
    arecv,
    azrecv,
    hbuf,
    hrecv,
    hyrecv,
    fbuf,
    frecv,
    fzrecv,
    bbuf,
    brecv,
    byrecv,
    cbuf,
    crecv,
    czrecv,
    send_sem,
    recv_sem,
    load_sem,
):
    d_model = nz * 2 * SLAB
    rows_l = d_model // 128
    dp, mp, pre = lax.axis_index("dp"), lax.axis_index("mp"), lax.axis_index("pre")
    z, xl, c = dp // 4, (dp // 2) % 2, dp % 2
    a = mp * ny + pre
    b = z * 2 + xl
    core_peer = (dp + 1 - 2 * c, mp, pre)
    x_peer = (dp + 2 - 4 * xl, mp, pre)
    hi_peer = (dp, 1 - mp, pre)
    cross_peer = (dp + 3 - 4 * xl - 2 * c, mp, pre)
    quad = (core_peer, x_peer, cross_peer)

    turn = (z - a // 2 + ny // 2 + nz) % nz
    goal_hi = jnp.where(xl == a % 2, mp, 1 - mp)
    flip_to = (a * 2 + c, goal_hi, (pre + turn) % ny)
    came = (z + pre - b % ny + ny // 2 + nz) % nz
    came_lo = jnp.where(mp == b // ny, xl, 1 - xl)
    flip_from = (came * 4 + came_lo * 2 + c, b // ny, b % ny)
    flip_to_2 = (a * 2 + c, 1 - goal_hi, (pre + turn) % ny)
    flip_from_2 = (came * 4 + (1 - came_lo) * 2 + c, b // ny, b % ny)

    def z_at(o):
        return (z + o) % nz

    def z_peer(o):
        return (z_at(o) * 4 + xl * 2 + c, mp, pre)

    def y_at(o):
        return (pre + o) % ny

    def y_peer(o):
        return (dp, mp, y_at(o))

    net = Net(send_sem, recv_sem)

    barrier = pltpu.get_barrier_semaphore()

    def greet(device):
        pl.semaphore_signal(barrier, inc=1, device_id=device, device_id_type=MESH)

    loads = []

    def load(src, dst):
        copy = pltpu.make_async_copy(src, dst, load_sem.at[len(loads)])
        copy.start()
        loads.append(copy)
        return copy

    def act_cols(o):
        return pl.ds(pl.multiple_of(z_at(o) * 128, 128), 128)

    z_order = far_first(nz) + [0]
    dy_load = load(dy_hbm, dy)
    act_loads = [load(act_hbm.at[:, act_cols(o)], act.at[i]) for i, o in enumerate(z_order)]
    other_loads = [
        load(left_hbm, left_old),
        load(right_hbm, right_old),
        load(p_left_hbm, p_left),
        load(p_right_hbm, p_right),
    ]

    greet(core_peer)
    greet(x_peer)
    greet(hi_peer)
    greet(cross_peer)
    for o in range(1, nz):
        greet(z_peer(o))
    for o in range(1, ny):
        greet(y_peer(o))

    greet(flip_from)
    greet(flip_from_2)

    def slab_rows(z_, xl_):
        return pl.ds(pl.multiple_of((z_ * 2 + xl_) * SLAB, SLAB), SLAB)

    def pair_rows(z_):
        return pl.ds(pl.multiple_of(z_ * 2 * SLAB, 2 * SLAB), 2 * SLAB)

    def half_cols(c_):
        return pl.ds(pl.multiple_of(c_ * HALF, HALF), HALF)

    mine, other = half_cols(c), half_cols(1 - c)

    class Scatter:
        def __init__(self, part, rc, xs, rx, zs, rz):
            self.part, self.rc, self.xs, self.rx, self.zs, self.rz = part, rc, xs, rx, zs, rz
            self.ic = [net.slot() for _ in range(nz)]
            self.ix = [net.slot() for _ in range(nz)]
            self.iz = [net.slot() for _ in range(nz)]

        def block(self, o, value):
            rows = pair_rows(z_at(o))
            self.part[rows, :] = value
            net.send(self.ic[o], self.part.at[rows, other], self.rc.at[rows, :], core_peer)

        def over_x(self, o):
            rows = pair_rows(z_at(o))
            net.arrive(self.ic[o], self.rc.at[rows, :], core_peer)
            theirs = slab_rows(z_at(o), 1 - xl)
            self.xs[o] = self.part[theirs, mine] + self.rc[theirs, :]
            net.send(self.ix[o], self.xs.at[o], self.rx.at[o], x_peer)

        def over_z(self, o):
            net.arrive(self.ix[o], self.rx.at[o], x_peer)
            ours = slab_rows(z_at(o), xl)
            self.zs[o] = self.part[ours, mine] + self.rc[ours, :] + self.rx[o]
            if o:
                net.send(self.iz[o], self.zs.at[o], self.rz.at[o], z_peer(o))

        def total(self):
            value = self.zs[0]
            for o in near_first(nz):
                net.arrive(self.iz[o], self.rz.at[o], z_peer(o))
                value = value + self.rz[o]
            return value

    mixed = near_first(nz)[:2] + [o for o in far_first(nz) if o not in near_first(nz)[:2]]

    class Gather:
        def __init__(self, full):
            self.full = full
            self.ic = [net.slot() for _ in range(nz)]
            self.ix = [net.slot() for _ in range(nz)]
            self.iz = [net.slot() for _ in range(nz)]

        def over_z(self, value):
            rows = slab_rows(z, xl)
            self.full[rows, mine] = value
            chunk = self.full.at[rows, mine]
            net.send(self.ix[0], chunk, chunk, x_peer)
            for o in mixed:
                net.send(self.iz[o], chunk, chunk, z_peer(o))

        def over_x(self, o):
            chunk = self.full.at[slab_rows(z_at(nz - o), xl), mine]
            net.arrive(self.iz[o], chunk, z_peer(nz - o))
            net.send(self.ix[o], chunk, chunk, x_peer)

        def over_core(self, o):
            z_ = z_at(nz - o)
            net.arrive(self.ix[o], self.full.at[slab_rows(z_, 1 - xl), mine], x_peer)
            pair = self.full.at[pair_rows(z_), mine]
            net.send(self.ic[o], pair, pair, core_peer)

        def landed(self, o):
            net.arrive(self.ic[o], self.full.at[pair_rows(z_at(nz - o)), other], core_peer)

    class Sum:
        def __init__(self, buf, recv, zrecv):
            self.buf, self.recv, self.zrecv = buf, recv, zrecv
            self.iq = [net.slot() for _ in quad]
            self.iz = [net.slot() for _ in range(nz)]

        def over_quad(self):
            for i, peer in zip(self.iq, quad):
                net.send(i, self.buf.at[0], self.recv.at[i - self.iq[0]], peer)

        def over_z(self):
            value = self.buf[0]
            for i, peer in zip(self.iq, quad):
                net.arrive(i, self.recv.at[i - self.iq[0]], peer)
                value = value + self.recv[i - self.iq[0]]
            self.buf[1] = value
            for o in far_first(nz):
                net.send(self.iz[o], self.buf.at[1], self.zrecv.at[o], z_peer(o))

        def total(self):
            value = self.buf[1]
            for o in near_first(nz):
                net.arrive(self.iz[o], self.zrecv.at[o], z_peer(o))
                value = value + self.zrecv[o]
            return value

    class SumA:
        def __init__(self, buf, recv, yrecv):
            self.buf, self.recv, self.yrecv = buf, recv, yrecv
            self.ix = net.slot()
            self.iy = [net.slot() for _ in range(ny)]

        def over_hi(self):
            net.send(self.ix, self.buf.at[0], self.recv, hi_peer)

        def over_y(self):
            net.arrive(self.ix, self.recv, hi_peer)
            self.buf[1] = self.buf[0] + self.recv[...]
            for o in far_first(ny):
                net.send(self.iy[o], self.buf.at[1], self.yrecv.at[o], y_peer(o))

        def total(self):
            value = self.buf[1]
            for o in near_first(ny):
                net.arrive(self.iy[o], self.yrecv.at[o], y_peer(o))
                value = value + self.yrecv[o]
            return value

    old_sum = Sum(abuf, arecv, azrecv)
    h_sum = SumA(hbuf, hrecv, hyrecv)
    image_sum = SumA(bbuf, brecv, byrecv)
    left_sum = Sum(fbuf, frecv, fzrecv)
    last_sum = Sum(cbuf, crecv, czrecv)

    first = Scatter(part, rc, xs, rx, zs, rz)
    gather = Gather(grad)

    def grad_block(i):
        act_loads[i].wait()
        return lax.dot_general(act[i], dy[...], TN, preferred_element_type=F32)

    def blocks_and_x(scatter, block_of, between=()):
        between = dict(between)
        for i in range(nz):
            scatter.block(z_order[i], block_of(i))
            if i in between:
                between[i]()
            if i >= 3:
                scatter.over_x(z_order[i - 3])
        for i in range(nz - 3, nz):
            if i >= 0:
                scatter.over_x(z_order[i])

    dy_load.wait()
    first_value = grad_block(0)
    pl.semaphore_wait(barrier, 6 + (nz - 1) + (ny - 1))
    blocks_and_x(first, lambda i: grad_block(i) if i else first_value)

    for copy in other_loads:
        copy.wait()
    row = lax.broadcasted_iota(jnp.int32, (8, 128), 0)
    p_row = jnp.broadcast_to(p_right[pl.ds(dp, 1), :], (8, 128))
    old_right = dot3(halves(p_row), halves(right_old[...]), NT)
    abuf[0] = jnp.where(row == 0, old_right[:, :HALF], old_right[:, HALF:])
    old_sum.over_quad()
    for z_ in range(nz):
        prod[slab_rows(z_, 1 - xl), :] = jnp.zeros((SLAB, HALF), F32)
    for o in z_order[: nz // 2]:
        first.over_z(o)
    for o in z_order[nz // 2 :]:
        first.over_z(o)
    old_sum.over_z()
    gown[...] = first.total()

    i_flip, i_flip_2 = net.slot(), net.slot()
    iy = [net.slot() for _ in range(ny)]
    ih = [net.slot() for _ in range(ny)]

    def panel_z(y_):
        return (z + y_ - b % ny + ny // 2 + nz) % nz

    def panel_slab(mp_, y_):
        return panel.at[slab_rows(panel_z(y_), jnp.where(mp_ == b // ny, xl, 1 - xl)), :]

    chunk = panel.at[slab_rows(z, xl), :]
    net.send(i_flip, gown, chunk, flip_to)
    net.send(i_flip_2, gown, chunk, flip_to_2)
    gather.over_z(gown[...])
    far = [o for o in far_first(ny) if min(o, ny - o) > 2]
    near = [o for o in far_first(ny) if min(o, ny - o) <= 2]
    net.arrive(i_flip, panel_slab(mp, pre), flip_from)
    for o in far:
        net.send(iy[o], panel_slab(mp, pre), panel_slab(mp, pre), y_peer(o))
    net.arrive(i_flip_2, panel_slab(1 - mp, pre), flip_from_2)
    own_pair = panel.at[pair_rows(panel_z(pre)), :]
    for o in near:
        net.send(iy[o], own_pair, own_pair, y_peer(o))
    for o in mixed:
        gather.over_x(o)
    core_order = [0] + mixed
    for o in core_order[: nz // 2 + 1]:
        gather.over_core(o)
    for o in reversed(far):
        slab = panel_slab(mp, y_at(ny - o))
        net.arrive(iy[o], slab, y_peer(ny - o))
        net.send(ih[o], slab, slab, hi_peer)
    for o in core_order[nz // 2 + 1 :]:
        gather.over_core(o)
    for o in core_order:
        gather.landed(o)

    il = [net.slot() for _ in range(ny)]
    ilx = net.slot()
    ilg = [net.slot() for _ in range(ny)]
    own32 = pl.ds(pl.multiple_of(dp * 32, 32), 32)
    grad_split = halves(grad[...])
    probe_a = jnp.concatenate([p_right[pl.ds(2 * a, 1), :], p_right[pl.ds(2 * a + 1, 1), :]], axis=1)
    rows40 = jnp.concatenate([grad[own32, :], jnp.broadcast_to(probe_a, (8, 2 * HALF))], axis=0)
    both = dot3(halves(rows40), grad_split, NT)
    for j in range(rows_l):
        hbuf[0, pl.ds(j, 1), :] = both[32:33, j * 128 : (j + 1) * 128]
    h_sum.over_hi()
    lpart[...] = both[0:32, :] * (1.0 / ff)
    old_lanes = pl.ds(pl.multiple_of((a // 2) * 128, 128), 128)
    old = left_old[...] * DECAY
    side = lax.broadcasted_iota(jnp.int32, (32, 128), 1) // SLAB
    lpart[:, old_lanes] += jnp.where(side == a % 2, jnp.concatenate([old, old], axis=1), 0.0)

    def l_lanes(y_):
        return pl.ds(pl.multiple_of(y_ * 128, 128), 128)

    for o in far_first(ny):
        net.send(il[o], lpart.at[:, l_lanes(y_at(o))], lr.at[o], y_peer(o))
    for o in near:
        net.arrive(iy[o], panel.at[pair_rows(panel_z(y_at(ny - o))), :], y_peer(ny - o))
    for o in reversed(far):
        net.arrive(ih[o], panel_slab(1 - mp, y_at(ny - o)), hi_peer)

    gram = dot3(halves(panel[...].T), grad_split, NN)
    rtile[...] = right_old[...].T * DECAY + gram * (1.0 / d_model)
    rt_split = halves(rtile[...])
    h_sum.over_y()

    second = Scatter(part2, rc2, xs2, rx2, zs2, rz2)

    def prod_block(i):
        return dot3(halves(panel[pair_rows(z_at(z_order[i])), :]), rt_split, NN)

    def right_images():
        h = h_sum.total()
        h_row = jnp.concatenate([h[j : j + 1, :] for j in range(rows_l)], axis=1)
        new = dot3(halves(jnp.broadcast_to(h_row, (8, d_model))), grad_split, NN)
        old_image = old_sum.total()
        f_old = jnp.concatenate([old_image[0:1, :], old_image[1:2, :]], axis=1)
        f_row = f_old * DECAY + new[0:1, :] * (1.0 / d_model)
        square = jnp.sum(f_row * f_row, axis=1, keepdims=True)
        image = dot3(halves(jnp.broadcast_to(f_row, (8, 2 * HALF))), rt_split, NT)
        bbuf[0] = jnp.where(row == 0, image, square)
        image_sum.over_hi()

    def left_rows():
        total = lpart[:, l_lanes(pre)]
        for o in near_first(ny):
            net.arrive(il[o], lr.at[o], y_peer(o))
            total = total + lr[o]
        lsum[...] = total
        net.send(ilx, lsum, lx, hi_peer)

    blocks_and_x(second, prod_block)
    left_rows()
    cut = [5, 6, 8] if nz > 7 else [1, 1, 1]
    for o in z_order[: cut[0]]:
        second.over_z(o)
    right_images()
    for o in z_order[cut[0] : cut[1]]:
        second.over_z(o)
    net.arrive(ilx, lx, hi_peer)
    lrow[:, l_lanes(pre)] = lsum[...] + lx[...]
    own_lanes = lrow.at[:, l_lanes(pre)]
    for o in far_first(ny):
        net.send(ilg[o], own_lanes, own_lanes, y_peer(o))
    for o in z_order[cut[1] : cut[2]]:
        second.over_z(o)
    image_sum.over_y()
    for o in z_order[cut[2] :]:
        second.over_z(o)


    iz2 = [net.slot() for _ in range(nz)]
    i_prod = net.slot()
    i_term = [net.slot() for _ in quad]
    prod[slab_rows(z, xl), :] = second.total()
    own_prod = prod.at[slab_rows(z, xl), :]
    for o in far_first(nz):
        net.send(iz2[o], own_prod, own_prod, z_peer(o))

    def rows_of(c_):
        return pl.ds(pl.multiple_of((z * 2 + xl) * SLAB + c_ * 32, 32), 32)

    net.send(i_prod, prod.at[rows_of(1 - c), :], wrow, core_peer)

    for o in near_first(ny):
        net.arrive(ilg[o], lrow.at[:, l_lanes(y_at(ny - o))], y_peer(ny - o))

    def l_rows(xl_, c_):
        return lrows.at[pl.ds(pl.multiple_of((xl_ * 2 + c_) * 32, 32), 32), :]

    i_rows, i_rows_x, i_rows_xc = net.slot(), net.slot(), net.slot()
    net.send(i_rows_x, lrow, l_rows(xl, c), x_peer)
    net.send(i_rows, lrow, l_rows(xl, c), core_peer)
    l_rows(xl, c)[...] = lrow[...]
    f_left = jnp.zeros((32, 1), F32)
    for j in range(rows_l):
        f_left = f_left + jnp.sum(
            lrow[:, j * 128 : (j + 1) * 128] * p_left[pl.ds(j, 1), :], axis=1, keepdims=True
        )
    left_image = jnp.sum(lrow[...] * f_left, axis=0, keepdims=True)
    for j in range(rows_l):
        fbuf[0, pl.ds(j, 1), :] = left_image[:, j * 128 : (j + 1) * 128]
    left_square = jnp.sum(f_left * f_left, axis=0, keepdims=True)
    fbuf[0, pl.ds(rows_l, 8), :] = jnp.broadcast_to(left_square, (8, 128))
    left_sum.over_quad()

    whole = image_sum.total()
    norm_right = jnp.sqrt(whole[1:2, 0:1] + FLOOR)
    scaled = whole[0:1, :] / norm_right
    right_part = jnp.sum(scaled * scaled, axis=1, keepdims=True)
    cbuf[0] = jnp.broadcast_to(right_part, (8, 128))
    last_sum.over_quad()

    left_grad = dot3(halves(lrow[...]), grad_split, NN)
    right_out[...] = rtile[...].T
    lanes = lrow[:, old_lanes]
    left_out[...] = jnp.where(a % 2 == 0, lanes[:, :SLAB], lanes[:, SLAB:])
    left_sum.over_z()
    last_sum.over_z()
    net.arrive(i_rows_x, l_rows(1 - xl, c), x_peer)
    net.send(i_rows_xc, l_rows(1 - xl, c), l_rows(1 - xl, c), core_peer)
    net.arrive(i_rows, l_rows(xl, 1 - c), core_peer)
    net.arrive(i_rows_xc, l_rows(1 - xl, 1 - c), core_peer)

    term = jnp.zeros((128, HALF), F32)
    for o in [0] + [nz - o for o in far_first(nz)]:
        z_ = z_at(o)
        if o:
            net.arrive(iz2[nz - o], prod.at[slab_rows(z_, xl), :], z_peer(o))
        term = term + dot3(
            halves(lrows[:, l_lanes(z_)]), halves(prod[pair_rows(z_), :]), NN
        )
    terms[...] = term

    def term_rows(xl_, c_):
        return pl.ds(pl.multiple_of((xl_ * 2 + c_) * 32, 32), 32)

    net.send(i_term[1], terms.at[term_rows(1 - xl, c), :], tx, x_peer)
    net.send(i_term[2], terms.at[term_rows(1 - xl, 1 - c), :], tcross, cross_peer)
    net.send(i_term[0], terms.at[term_rows(xl, 1 - c), :], tcore, core_peer)
    top_right = jnp.sqrt(last_sum.total()[0:1, 0:1] + FLOOR)
    images = left_sum.total()
    norm_left = jnp.sqrt(images[rows_l : rows_l + 1, 0:1] + FLOOR)
    unit_image = images[0:rows_l, :] / norm_left
    top_left = jnp.sqrt(
        jnp.sum(jnp.sum(unit_image * unit_image, axis=1, keepdims=True), axis=0, keepdims=True)
        + FLOOR
    )
    scale = lax.rsqrt(jnp.sqrt(top_left * top_right)) * 0.0625
    rest = 5.0 * (5.0 * grad[own32, :] - left_grad / top_left)
    update_out[...] = rest
    net.arrive(i_prod, wrow, core_peer)
    net.arrive(i_term[0], tcore, core_peer)
    net.arrive(i_term[1], tx, x_peer)
    by_right = ((terms[term_rows(xl, c), :] + tx[...]) / top_left - 5.0 * prod[rows_of(c), :]) / top_right
    update_out[:, mine] = (update_out[:, mine] + by_right) * scale
    net.arrive(i_term[2], tcross, cross_peer)
    by_right = ((tcore[...] + tcross[...]) / top_left - 5.0 * wrow[...]) / top_right
    update_out[:, other] = (update_out[:, other] + by_right) * scale

    net.finish()


def store(left, right, update, left_out, right_out, update_out, sem):
    pairs = ((left, left_out), (right, right_out), (update, update_out))
    copies = [pltpu.make_async_copy(src, dst, sem.at[i]) for i, (src, dst) in enumerate(pairs)]
    for copy in copies:
        copy.start()
    for copy in copies:
        copy.wait()


def step(nz, ny, ff, activations, grad_output, left_old, right_old, probe_left, probe_right):
    d_model = activations.shape[1]
    block = grad_output.shape[1]
    rows_l = d_model // 128
    vmem = pltpu.VMEM

    def scatter_bufs(columns):
        return [
            vmem((d_model, block), F32),
            vmem((d_model, HALF), F32),
            vmem((nz, SLAB, HALF), F32),
            vmem((nz, SLAB, HALF), F32),
            vmem((nz, SLAB, HALF), F32),
            vmem((nz, SLAB, HALF), F32),
            vmem((d_model, columns), F32),
        ]

    scratch = [
        vmem((nz, activations.shape[0], 128), BF16),
        vmem(grad_output.shape, BF16),
        vmem((left_old.shape[1], left_old.shape[0]), F32),
        vmem(right_old.shape, F32),
        vmem((probe_left.shape[0] // 128, 128), F32),
        vmem((probe_right.shape[0] // 128, 128), F32),
        *scatter_bufs(block),
        *scatter_bufs(HALF),
        vmem((SLAB, HALF), F32),
        vmem((d_model, HALF), F32),
        vmem((HALF, block), F32),
        vmem((32, d_model), F32),
        vmem((ny, 32, 128), F32),
        vmem((32, 128), F32),
        vmem((32, 128), F32),
        vmem((32, d_model), F32),
        vmem((128, d_model), F32),
        vmem((128, HALF), F32),
        vmem((32, HALF), F32),
        vmem((32, HALF), F32),
        vmem((32, HALF), F32),
        vmem((32, HALF), F32),
        vmem((2, 8, 128), F32),
        vmem((3, 8, 128), F32),
        vmem((nz, 8, 128), F32),
        vmem((2, rows_l, 128), F32),
        vmem((rows_l, 128), F32),
        vmem((ny, rows_l, 128), F32),
        vmem((2, rows_l + 8, 128), F32),
        vmem((3, rows_l + 8, 128), F32),
        vmem((nz, rows_l + 8, 128), F32),
        vmem((2, 8, 128), F32),
        vmem((8, 128), F32),
        vmem((ny, 8, 128), F32),
        vmem((2, 8, 128), F32),
        vmem((3, 8, 128), F32),
        vmem((nz, 8, 128), F32),
        pltpu.SemaphoreType.DMA((COPIES,)),
        pltpu.SemaphoreType.DMA((COPIES,)),
        pltpu.SemaphoreType.DMA((nz + 5,)),
    ]
    spec = pl.BlockSpec(memory_space=pltpu.VMEM)
    left, right, update = pl.pallas_call(
        functools.partial(kernel, nz, ny, ff),
        out_shape=(
            jax.ShapeDtypeStruct((left_old.shape[1], left_old.shape[0]), F32),
            jax.ShapeDtypeStruct(right_old.shape, F32),
            jax.ShapeDtypeStruct((d_model // (4 * nz), block), F32),
        ),
        in_specs=[pl.BlockSpec(memory_space=pltpu.HBM)] * 6,
        out_specs=(spec,) * 3,
        scratch_shapes=scratch,
        compiler_params=pltpu.CompilerParams(
            collective_id=0, has_side_effects=True, vmem_limit_bytes=58 * 1024 * 1024
        ),
        name="shampoo",
    )(
        activations,
        grad_output,
        left_old.T,
        right_old,
        probe_left.reshape(-1, 128),
        probe_right.reshape(-1, 128),
    )
    left, right, update = pl.pallas_call(
        store,
        out_shape=tuple(jax.ShapeDtypeStruct(r.shape, F32) for r in (left, right, update)),
        in_specs=[spec] * 3,
        out_specs=(pl.BlockSpec(memory_space=pltpu.HBM),) * 3,
        scratch_shapes=[pltpu.SemaphoreType.DMA((3,))],
        name="store",
    )(left, right, update)
    return left.T, right, update


def solution(mesh):
    nz = mesh.shape["dp"] // 4
    ny = mesh.shape["pre"]
    in_specs = (
        P("dp", None),
        P("dp", ("mp", "pre")),
        P(("mp", "pre"), "dp"),
        P(("mp", "pre"), "dp"),
        P(),
        P(),
    )
    out_specs = (P(("mp", "pre"), "dp"), P(("mp", "pre"), "dp"), P("dp", ("mp", "pre")))
    ff = 2 * ny * 2 * HALF
    return jax.shard_map(
        functools.partial(step, nz, ny, ff),
        mesh=mesh,
        in_specs=in_specs,
        out_specs=out_specs,
        check_vma=False,
    )
```
